32 devices in a mesh: probe: 4 (over y, x), mp: 8 (over z, core).
Axes of the slice: x: 2, y: 2, z: 4, core: 2. Of those that a mesh axis runs over, the one named last changes fastest.
Arguments:
- tokens: bfloat16 [512, 2048], P('mp'), may hold values from -6 to 6
- targets: bfloat16 [512, 2048], P('mp'), may hold values from -6 to 6
- norm_gain: float32 [2048], replicated, may hold values from 0.5 to 1.5
- weights: bfloat16 [3, 5120, 2048], P(None, 'mp'), may hold values from -0.125 to 0.125
- probe_signs: bfloat16 [4, 3, 5120, 2048], P('probe', None, 'mp'), may hold values from -1 to 1, as said below
- m_state: float32 [3, 5120, 2048], P(None, 'mp'), may hold values from -0.3 to 0.3
- v_state: float32 [3, 2560, 16], P(None, 'mp'), may hold values from 0.0001 to 0.003
Outputs:
- hess_blocks: float32 [3, 2560, 16], P(None, 'mp')
- new_moment: float32 [3, 5120, 2048], P(None, 'mp')
- new_curvature: float32 [3, 2560, 16], P(None, 'mp')
- update: float32 [3, 5120, 2048], P(None, 'mp')
The draws below stay inside these ranges and needn't reach their ends.
Inputs may be any that keep to these rules, and one draw needn't show every extreme that they name: `probe_signs`: every entry is +1 or -1, independently.
All inputs are finite; a program needn't handle non-finite values.
Results may differ from the reference program's by a relative error of at most 0.0026.
Values may be sent and summed in bfloat16 or wider, within the bound.
No kernel may reach another device: no remote copies, remote signals or barrier semaphores. Data moves between devices by JAX's collectives and lax.ppermute only.
A program may use at most 128 MiB of HBM per device.

```python
import math
import jax
import jax.numpy as jnp
from jax import lax

D = 2048
FF = 5120
TOKENS = 512
BLOCK_ROWS = 2
BLOCK_COLS = 128
STEP = 4
PROBES = 4


def draw_probe_signs(key, part):
    signs = jax.random.rademacher(key, (PROBES, 3, FF, D), dtype=jnp.float32)
    return signs.astype(jnp.bfloat16)


def steps_of(key, dims, pieces, low, high):
    loudness, own = 1.0, jax.random.fold_in(key, 6)
    for axis_at, blocks in pieces:
        heights = jnp.exp(jax.random.uniform(jax.random.fold_in(own, axis_at), (blocks,), jnp.float32, low / len(pieces), high / len(pieces)))
        loudness = loudness * jnp.repeat(heights, dims[axis_at] // blocks).reshape([-1 if axis == axis_at else 1 for axis in range(len(dims))])
    return loudness


def centred(own_key, dims, spread, bound, pieces=(), held_as=jnp.bfloat16):
    loudness = steps_of(own_key, dims, pieces, -0.22, 0.18) if pieces else 1.0
    values = jax.random.normal(own_key, dims, jnp.float32) * spread * loudness
    return jnp.minimum(jnp.maximum(values, -bound), bound).astype(held_as)


def setup_inputs(seed: int = 0) -> dict:
    streams_of = jax.random.split(jax.random.key(seed), 8)
    tokens = centred(streams_of[0], (TOKENS, D), 1.0, 6.0, ((0, 8),))
    targets = centred(streams_of[1], (TOKENS, D), 1.0, 6.0, ((0, 8),))
    norm_gain = jnp.clip(1.0 + 0.1 * jax.random.normal(streams_of[2], (D,), jnp.float32), 0.5, 1.5)
    weights = centred(streams_of[3], (3, FF, D), D ** -0.5, 0.125, ((1, 8),))
    probe_signs = draw_probe_signs(jax.random.fold_in(streams_of[7], 71), 0)
    m_state = centred(streams_of[5], (3, FF, D), 0.05, 0.3, ((1, 8),), jnp.float32)
    v_state = jnp.clip(jnp.exp(math.log(0.003) - 3.4011974 * jax.random.uniform(streams_of[6], (3, FF // BLOCK_ROWS, D // BLOCK_COLS), jnp.float32) ** steps_of(streams_of[6], (3, FF // BLOCK_ROWS, D // BLOCK_COLS), ((1, 8),), -0.2, 0.2)), 0.0001, 0.003)
    return {"tokens": tokens, "targets": targets, "norm_gain": norm_gain, "weights": weights, "probe_signs": probe_signs, "m_state": m_state, "v_state": v_state}


beta_one = 0.9
beta_two = 0.999
epsilon = 0.0001
root_half = 0.7978845608028654
cubic = 0.044715

def gelu_parts(value):
    inner = root_half * (value + cubic * value * value * value)
    slope_inner = root_half * (1.0 + 3.0 * cubic * value * value)
    curve_inner = 6.0 * root_half * cubic * value
    tangent = jnp.tanh(inner)
    damping = 1.0 - tangent * tangent
    activated = 0.5 * value * (1.0 + tangent)
    slope = 0.5 * (1.0 + tangent) + 0.5 * value * damping * slope_inner
    bend = damping * slope_inner + 0.5 * value * damping * (curve_inner - 2.0 * tangent * slope_inner * slope_inner)
    return (activated, slope, bend)

def times_rows(left, weight):
    return lax.dot_general(left, weight, (((1,), (1,)), ((), ())), preferred_element_type=jnp.float32)

def outer_sum(left, right):
    return lax.dot_general(left, right, (((0,), (0,)), ((), ())), preferred_element_type=jnp.float32)

def block_mean(values):
    height, width = values.shape
    return values.reshape(height // BLOCK_ROWS, BLOCK_ROWS, width // BLOCK_COLS, BLOCK_COLS).mean(axis=(1, 3))

def adam_parts(grads, hess, m_state, v_state):
    new_m = beta_one * m_state + (1.0 - beta_one) * grads
    new_v = beta_two * v_state + (1.0 - beta_two) * hess * hess
    denom = jnp.sqrt(new_v / (1.0 - beta_two ** STEP)) + epsilon
    kinds, height, width = new_m.shape
    shaped = new_m.reshape(kinds, height // BLOCK_ROWS, BLOCK_ROWS, width // BLOCK_COLS, BLOCK_COLS)
    update = shaped / (1.0 - beta_one ** STEP) / denom[:, :, None, :, None]
    return (new_m, new_v, update.reshape(kinds, height, width))

def reference(tokens, targets, norm_gain, weights, probe_signs, m_state, v_state):
    count = tokens.shape[0]
    whole_x = tokens.astype(jnp.float32)
    factor = lax.rsqrt(lax.optimization_barrier(jnp.mean(whole_x * whole_x, axis=-1, keepdims=True)) + 1e-06)
    normed = (whole_x * factor * norm_gain).astype(jnp.bfloat16)
    w_gate, w_up, w_out = (weights[0], weights[1], weights[2])
    pre_gate = times_rows(normed, w_gate)
    pre_up = times_rows(normed, w_up)
    activated, slope, bend = gelu_parts(pre_gate)
    hidden = (activated * pre_up).astype(jnp.bfloat16)
    resid = whole_x + jnp.dot(hidden, w_out, preferred_element_type=jnp.float32) - targets.astype(jnp.float32)
    dout = (resid / count).astype(jnp.bfloat16)
    dhid = times_rows(dout, w_out)
    dgate = (dhid * pre_up * slope).astype(jnp.bfloat16)
    dup = (dhid * activated).astype(jnp.bfloat16)
    grads = jnp.stack([outer_sum(dgate, normed), outer_sum(dup, normed), outer_sum(hidden, dout)])
    total = jnp.zeros(v_state.shape, jnp.float32)
    for index in range(probe_signs.shape[0]):
        sign_gate = probe_signs[index, 0]
        sign_up = probe_signs[index, 1]
        sign_out = probe_signs[index, 2]
        tan_gate = times_rows(normed, sign_gate)
        tan_up = times_rows(normed, sign_up)
        tan_hid = (slope * tan_gate * pre_up + activated * tan_up).astype(jnp.bfloat16)
        tan_res = jnp.dot(tan_hid, w_out, preferred_element_type=jnp.float32) + jnp.dot(hidden, sign_out, preferred_element_type=jnp.float32)
        tan_dout = (tan_res / count).astype(jnp.bfloat16)
        tan_dhid = times_rows(tan_dout, w_out) + times_rows(dout, sign_out)
        tan_dgate = ((tan_dhid * pre_up + dhid * tan_up) * slope + dhid * pre_up * bend * tan_gate).astype(jnp.bfloat16)
        tan_dup = (tan_dhid * activated + dhid * slope * tan_gate).astype(jnp.bfloat16)
        hv_gate = outer_sum(tan_dgate, normed)
        hv_up = outer_sum(tan_dup, normed)
        hv_out = outer_sum(tan_hid, dout) + outer_sum(hidden, tan_dout)
        total = total + jnp.stack([block_mean(sign_gate * hv_gate), block_mean(sign_up * hv_up), block_mean(sign_out * hv_out)])
    hess = total / probe_signs.shape[0]
    new_m, new_v, update = adam_parts(grads, hess, m_state, v_state)
    return (hess, new_m, new_v, update)
```

```python
import functools

import jax
import jax.numpy as jnp
from jax import lax
from jax.experimental import pallas as pl
from jax.experimental.pallas import tpu as pltpu
from jax.sharding import PartitionSpec as P


BLOCK_ROWS = 2
BLOCK_COLS = 128
STEP = 4

beta_one = 0.9
beta_two = 0.999
epsilon = 0.0001
root_half = 0.7978845608028654
cubic = 0.044715

F32 = jnp.float32
BF16 = jnp.bfloat16


def gelu_parts(value):
    square = value * value
    inner = root_half * (value + cubic * square * value)
    slope_inner = root_half * (1.0 + 3.0 * cubic * square)
    curve_inner = 6.0 * root_half * cubic * value
    tangent = jnp.tanh(inner)
    damping = 1.0 - tangent * tangent
    activated = 0.5 * value * (1.0 + tangent)
    slope = 0.5 * (1.0 + tangent) + 0.5 * value * damping * slope_inner
    bend = damping * slope_inner + 0.5 * value * damping * (
        curve_inner - 2.0 * tangent * slope_inner * slope_inner
    )
    return (activated, slope, bend)


def dot_nt(left, right):
    return lax.dot_general(left, right, (((1,), (1,)), ((), ())), preferred_element_type=F32)


def dot_tn(left, right):
    return lax.dot_general(left, right, (((0,), (0,)), ((), ())), preferred_element_type=F32)


def dot_nn(left, right):
    return jnp.dot(left, right, preferred_element_type=F32)


def unit_block(units):
    return 128 if units % 128 == 0 else units


def whole(shape):
    zeros = (0,) * len(shape)
    return pl.BlockSpec(shape, lambda *_: zeros)


def call(body, name, grid, in_specs, out_specs, out_shape, scratch, flops, traffic, args):
    return pl.pallas_call(
        body,
        name=name,
        grid=grid,
        in_specs=in_specs,
        out_specs=out_specs,
        out_shape=out_shape,
        scratch_shapes=scratch,
        compiler_params=pltpu.CompilerParams(
            dimension_semantics=("arbitrary",) * len(grid), vmem_limit_bytes=60 * 1024 * 1024
        ),
        cost_estimate=pl.CostEstimate(flops=flops, bytes_accessed=traffic, transcendentals=0),
    )(*args)


def column_sums(values):
    rows, width = values.shape
    lanes = lax.broadcasted_iota(jnp.int32, (rows, 128), 1)
    out = jnp.zeros((rows, 128), F32)
    for at in range(width // BLOCK_COLS):
        part = values[:, at * BLOCK_COLS : (at + 1) * BLOCK_COLS]
        out = jnp.where(lanes == at, jnp.sum(part, axis=1, keepdims=True), out)
    return out.T[: width // BLOCK_COLS]


def norm_kernel(tokens, gain, out):
    x = tokens[...].astype(F32)
    factor = lax.rsqrt(jnp.mean(x * x, axis=-1, keepdims=True) + 1e-06)
    out[...] = (x * factor * gain[...]).astype(BF16)


def norm(tokens, gain):
    rows, width = tokens.shape
    return call(
        norm_kernel,
        "norm",
        (1,),
        [whole((rows, width)), whole((1, width))],
        whole((rows, width)),
        jax.ShapeDtypeStruct((rows, width), BF16),
        [],
        rows * width * 4,
        rows * width * 4,
        (tokens, gain.reshape(1, width)),
    )


def forward_kernel(pieces, refs):
    blocks = refs[:pieces]
    (w, z, normed_out, p_out, g_out, q_out, s_out, hid_out, tan_out) = refs[pieces : pieces + 9]
    (own_q, sib_q, own_t, sib_t, x, acc, acc_q) = refs[pieces + 9 :]
    step = pl.program_id(0)
    rows = blocks[0].shape[0]

    @pl.when(step == 0)
    def _():
        for at in range(pieces):
            x[at * rows : (at + 1) * rows] = blocks[at][...]
        normed_out[...] = x[...]

    units, width = w.shape[1:]
    pre = dot_nt(w[0:2].reshape(2 * units, width), x[...])
    tan = dot_nt(z[0, 0:2].reshape(2 * units, width), x[...])
    pre_gate, pre_up = (pre[:units], pre[units:])
    tan_gate, tan_up = (tan[:units], tan[units:])
    activated, slope, bend = gelu_parts(pre_gate)
    p = pre_up * slope
    p_out[...] = p
    g_out[...] = activated
    q_out[...] = tan_up * slope + pre_up * bend * tan_gate
    s_out[...] = slope * tan_gate
    hidden = (activated * pre_up).astype(BF16)
    tan_hid = (p * tan_gate + activated * tan_up).astype(BF16)
    hid_out[...] = hidden
    tan_out[...] = tan_hid
    quarter = acc_q.shape[1]
    first = pl.multiple_of(lax.axis_index("probe") * quarter, quarter)
    left = jnp.concatenate([tan_hid, hidden], axis=0)
    right = jnp.concatenate([w[2], z[0, 2]], axis=0)
    add_q = dot_tn(hidden, w[2, :, pl.ds(first, quarter)])
    add_t = dot_tn(left, right)

    @pl.when(step == 0)
    def _():
        acc_q[...] = add_q
        acc[...] = add_t

    @pl.when(step > 0)
    def _():
        acc_q[...] += add_q
        acc[...] += add_t

    @pl.when(step == pl.num_programs(0) - 1)
    def _():
        half = own_q.shape[0]
        own_q[...] = acc_q[:half]
        own_t[...] = acc[:half]
        sib_q[...] = acc_q[half:].astype(sib_q.dtype)
        sib_t[...] = acc[half:].astype(sib_t.dtype)


def forward(blocks, weights, signs, quarter, sib_type):
    rows, width = blocks[0].shape
    count = rows * len(blocks)
    kinds, units, _ = weights.shape
    ub = unit_block(units)
    half = count // 2
    unit_spec = pl.BlockSpec((ub, count), lambda i: (i, 0))
    shape = jax.ShapeDtypeStruct
    return call(
        lambda *refs: forward_kernel(len(blocks), refs),
        "forward",
        (units // ub,),
        [whole((rows, width))] * len(blocks)
        + [
            pl.BlockSpec((kinds, ub, width), lambda i: (0, i, 0)),
            pl.BlockSpec((1, kinds, ub, width), lambda i: (0, 0, i, 0)),
        ],
        [whole((count, width))]
        + [unit_spec] * 6
        + [whole((half, quarter))] * 2
        + [whole((half, width))] * 2,
        [shape((count, width), BF16)]
        + [shape((units, count), F32)] * 4
        + [shape((units, count), BF16)] * 2
        + [
            shape((half, quarter), F32),
            shape((half, quarter), sib_type),
            shape((half, width), F32),
            shape((half, width), sib_type),
        ],
        [
            pltpu.VMEM((count, width), BF16),
            pltpu.VMEM((count, width), F32),
            pltpu.VMEM((count, quarter), F32),
        ],
        2 * count * units * width * 6,
        units * width * 12 + units * count * 20 + count * width * 12,
        (*blocks, weights, signs),
    )


def base_kernel(pieces, refs):
    blocks = refs[: 2 * pieces]
    (w, z, normed, p, g, q, s, hid, tan, m) = refs[2 * pieces : 2 * pieces + 10]
    (new_m, e_gate, e_up, sums, dout) = refs[2 * pieces + 10 :]
    step = pl.program_id(0)
    half, quarter = blocks[0].shape

    @pl.when(step == 0)
    def _():
        me = lax.axis_index("probe")
        for at in range(pieces):
            first = pl.multiple_of((me ^ at) * quarter, quarter)
            dout[:half, pl.ds(first, quarter)] = blocks[at][...]
            dout[half:, pl.ds(first, quarter)] = blocks[pieces + at][...]

    units = hid.shape[0]
    d = dout[...]
    both = dot_nt(jnp.concatenate([w[0], z[0, 0]], axis=0), d)
    dhid, sdhid = (both[:units], both[units:])
    pv, gv = (p[...], g[...])
    e_gate[...] = sdhid * pv + dhid * q[...]
    e_up[...] = sdhid * gv + dhid * s[...]
    inner = jnp.concatenate([(dhid * pv).astype(BF16), (dhid * gv).astype(BF16)], axis=0)
    grads = dot_nn(inner, normed[...])
    new_m[0] = beta_one * m[0] + (1.0 - beta_one) * grads[:units]
    new_m[1] = beta_one * m[1] + (1.0 - beta_one) * grads[units:]
    outer = dot_nn(jnp.concatenate([hid[...], tan[...]], axis=0), d)
    new_m[2] = beta_one * m[2] + (1.0 - beta_one) * outer[:units]
    sums[...] = column_sums(z[0, 0].astype(F32) * outer[units:])


def base(pieces, weights, signs, normed, p, g, q, s, hid, tan, m):
    half, quarter = pieces[0].shape
    count, width = normed.shape
    kinds, units, _ = weights.shape
    ub = unit_block(units)
    unit_spec = pl.BlockSpec((ub, count), lambda i: (i, 0))
    mat_spec = pl.BlockSpec((kinds, ub, width), lambda i: (0, i, 0))
    cols = width // BLOCK_COLS
    sum_spec = pl.BlockSpec((cols, ub), lambda i: (0, i))
    shape = jax.ShapeDtypeStruct
    return call(
        lambda *refs: base_kernel(len(pieces) // 2, refs),
        "base",
        (units // ub,),
        [whole((half, quarter))] * len(pieces)
        + [
            pl.BlockSpec((1, ub, width), lambda i: (2, i, 0)),
            pl.BlockSpec((1, 1, ub, width), lambda i: (0, 2, i, 0)),
            whole((count, width)),
        ]
        + [unit_spec] * 6
        + [mat_spec],
        [mat_spec, unit_spec, unit_spec, sum_spec],
        [
            shape((kinds, units, width), F32),
            shape((units, count), F32),
            shape((units, count), F32),
            shape((cols, units), F32),
        ],
        [pltpu.VMEM((count, width), BF16)],
        2 * count * units * width * 6,
        units * width * 28 + units * count * 28,
        (*pieces, weights, signs, normed, p, g, q, s, hid, tan, m),
    )


def tangent_kernel(pieces, refs):
    blocks = refs[:pieces]
    (w, z, normed, p, g, hid, e_gate, e_up, sums_in) = refs[pieces : pieces + 9]
    (sums, tdout) = refs[pieces + 9 :]
    step = pl.program_id(0)
    rows = blocks[0].shape[0]

    @pl.when(step == 0)
    def _():
        for at in range(pieces):
            tdout[at * rows : (at + 1) * rows] = blocks[at][...]

    units = hid.shape[0]
    t = tdout[...]
    tdh = dot_nt(w[0], t)
    inner = jnp.concatenate(
        [
            (tdh * p[...] + e_gate[...]).astype(BF16),
            (tdh * g[...] + e_up[...]).astype(BF16),
        ],
        axis=0,
    )
    hv = dot_nn(inner, normed[...])
    hv_out = dot_nn(hid[...], t)
    sums[0] = column_sums(z[0, 0].astype(F32) * hv[:units])
    sums[1] = column_sums(z[0, 1].astype(F32) * hv[units:])
    sums[2] = sums_in[...] + column_sums(z[0, 2].astype(F32) * hv_out)


def tangent(blocks, weights, signs, normed, p, g, hid, e_gate, e_up, sums):
    rows, width = blocks[0].shape
    count = normed.shape[0]
    kinds, units, _ = weights.shape
    ub = unit_block(units)
    unit_spec = pl.BlockSpec((ub, count), lambda i: (i, 0))
    cols = width // BLOCK_COLS
    return call(
        lambda *refs: tangent_kernel(len(blocks), refs),
        "tangent",
        (units // ub,),
        [whole((rows, width))] * len(blocks)
        + [
            pl.BlockSpec((1, ub, width), lambda i: (2, i, 0)),
            pl.BlockSpec((1, kinds, ub, width), lambda i: (0, 0, i, 0)),
            whole((count, width)),
        ]
        + [unit_spec] * 5
        + [pl.BlockSpec((cols, ub), lambda i: (0, i))],
        pl.BlockSpec((kinds, cols, ub), lambda i: (0, 0, i)),
        jax.ShapeDtypeStruct((kinds, cols, units), F32),
        [pltpu.VMEM((count, width), BF16)],
        2 * count * units * width * 4,
        units * width * 8 + units * count * 18,
        (*blocks, weights, signs, normed, p, g, hid, e_gate, e_up, sums),
    )


def update_kernel(probes, a, b, c, d, v, m, hess, new_v, update, rows):
    total = (a[0] + b[0]) + (c[0] + d[0])
    cols = total.shape[0]
    half = v.shape[1]
    rows[...] = jnp.concatenate([total, jnp.zeros((128 - cols, total.shape[1]), F32)], axis=0).T
    pair = rows[pl.ds(0, half, stride=2), :] + rows[pl.ds(1, half, stride=2), :]
    mean = pair * (1.0 / (BLOCK_ROWS * BLOCK_COLS * probes))
    h = mean[:, :cols]
    hess[0] = h
    nv = beta_two * v[0] + (1.0 - beta_two) * h * h
    new_v[0] = nv
    denom = jnp.sqrt(nv / (1.0 - beta_two**STEP)) + epsilon
    scale = 1.0 / (denom * (1.0 - beta_one**STEP))
    wide = jnp.concatenate([scale, jnp.zeros((half, 128 - cols), F32)], axis=1)
    rows[pl.ds(0, half, stride=2), :] = wide
    rows[pl.ds(1, half, stride=2), :] = wide
    full = rows[...]
    for at in range(cols):
        span = slice(at * BLOCK_COLS, (at + 1) * BLOCK_COLS)
        update[0, :, span] = m[0, :, span] * full[:, at : at + 1]


def update_step(sums, v, m):
    kinds, units, width = m.shape
    ub = unit_block(units)
    cols = width // BLOCK_COLS
    sum_spec = pl.BlockSpec((1, cols, ub), lambda k, i: (k, 0, i))
    v_spec = pl.BlockSpec((1, ub // BLOCK_ROWS, cols), lambda k, i: (k, i, 0))
    m_spec = pl.BlockSpec((1, ub, width), lambda k, i: (k, i, 0))
    shape = jax.ShapeDtypeStruct
    return call(
        functools.partial(update_kernel, len(sums)),
        "update",
        (kinds, units // ub),
        [sum_spec] * 4 + [v_spec, m_spec],
        [v_spec, v_spec, m_spec],
        [shape(v.shape, F32), shape(v.shape, F32), shape(m.shape, F32)],
        [pltpu.VMEM((ub, 128), F32)],
        units * width * 6,
        units * width * 24,
        (*sums, v, m),
    )


def to_sibling(x, chips):
    return lax.ppermute(x, "mp", [(i, i ^ 1) for i in range(2 * chips)])


def to_chip(x, chips, shift):
    pairs = [(2 * z + c, 2 * ((z + shift) % chips) + c) for z in range(chips) for c in range(2)]
    return lax.ppermute(x, "mp", pairs)


def to_probe(x, probes, flip):
    return lax.ppermute(x, "probe", [(i, i ^ flip) for i in range(probes)])


def gather_rows(x, chips):
    own = [x] + [to_chip(x, chips, shift) for shift in range(1, chips)]
    return own + [to_sibling(block, chips) for block in own]


def scatter_rows(own, sib, chips):
    rows = own.shape[0] // chips
    total = own + to_sibling(sib, chips).astype(F32)
    kept = total[:rows]
    for shift in range(1, chips):
        part = total[shift * rows : (shift + 1) * rows].astype(BF16)
        kept = kept + to_chip(part, chips, chips - shift).astype(F32)
    return kept


def shards(tokens, targets, norm_gain, weights, probe_signs, m_state, v_state):
    rows = tokens.shape[0]
    width = tokens.shape[1]
    members = lax.axis_size("mp")
    probes = lax.axis_size("probe")
    count = rows * members
    chips = members // 2
    near = chips <= 4
    quarter = width // probes
    first = lax.axis_index("probe") * quarter
    normed = norm(tokens, norm_gain)
    if near:
        blocks = gather_rows(normed, chips)
    else:
        blocks = [lax.all_gather(normed, "mp", axis=0, tiled=True)]
    (normed, p, g, q, s, hid, tan, own_q, sib_q, own_t, sib_t) = forward(
        blocks, weights, probe_signs, quarter, BF16 if near else F32
    )
    offset = lax.dynamic_slice_in_dim(tokens, first, quarter, 1).astype(
        F32
    ) - lax.dynamic_slice_in_dim(targets, first, quarter, 1).astype(F32)
    if near:
        part = ((scatter_rows(own_q, sib_q, chips) + offset) / count).astype(BF16)
        mine = jnp.concatenate(
            [part] + [to_chip(part, chips, shift) for shift in range(1, chips)], axis=0
        )
        pieces = [mine] + [to_probe(mine, probes, flip) for flip in range(1, probes)]
        pieces = pieces + [to_sibling(piece, chips) for piece in pieces]
        kept = scatter_rows(own_t, sib_t, chips)
        tan_dout = (kept / count).astype(BF16)
        tan_blocks = gather_rows(tan_dout, chips)
    else:
        part = lax.psum_scatter(
            jnp.concatenate([own_q, sib_q], axis=0), "mp", scatter_dimension=0, tiled=True
        )
        part = ((part + offset) / count).astype(BF16)
        mine = lax.all_gather(part, "mp", axis=0, tiled=True)
        pieces = [mine] + [to_probe(mine, probes, flip) for flip in range(1, probes)]
        half = count // 2
        pieces = [x[:half] for x in pieces] + [x[half:] for x in pieces]
        kept = lax.psum_scatter(
            jnp.concatenate([own_t, sib_t], axis=0), "mp", scatter_dimension=0, tiled=True
        )
        tan_dout = (kept / count).astype(BF16)
        tan_blocks = [lax.all_gather(tan_dout, "mp", axis=0, tiled=True)]
    new_m, e_gate, e_up, sums = base(
        pieces, weights, probe_signs, normed, p, g, q, s, hid, tan, m_state
    )
    sums = tangent(tan_blocks, weights, probe_signs, normed, p, g, hid, e_gate, e_up, sums)
    sums = [sums] + [to_probe(sums, probes, flip) for flip in range(1, probes)]
    hess, new_v, update = update_step(sums, v_state, new_m)
    return (hess, new_m, new_v, update)


def solution(mesh):
    return jax.shard_map(
        shards,
        mesh=mesh,
        in_specs=(
            P("mp", None),
            P("mp", None),
            P(),
            P(None, "mp", None),
            P("probe", None, "mp", None),
            P(None, "mp", None),
            P(None, "mp", None),
        ),
        out_specs=(
            P(None, "mp", None),
            P(None, "mp", None),
            P(None, "mp", None),
            P(None, "mp", None),
        ),
        check_vma=False,
    )
```

```python
import functools

import jax
import jax.numpy as jnp
from jax import lax
from jax.experimental import pallas as pl
from jax.experimental.pallas import tpu as pltpu
from jax.sharding import PartitionSpec as P


BLOCK_ROWS = 2
BLOCK_COLS = 128
STEP = 4

beta_one = 0.9
beta_two = 0.999
epsilon = 0.0001
root_half = 0.7978845608028654
cubic = 0.044715

F32 = jnp.float32
BF16 = jnp.bfloat16


def gelu_parts(value):
    square = value * value
    inner = root_half * (value + cubic * square * value)
    slope_inner = root_half * (1.0 + 3.0 * cubic * square)
    curve_inner = 6.0 * root_half * cubic * value
    tangent = jnp.tanh(inner)
    damping = 1.0 - tangent * tangent
    activated = 0.5 * value * (1.0 + tangent)
    slope = 0.5 * (1.0 + tangent) + 0.5 * value * damping * slope_inner
    bend = damping * slope_inner + 0.5 * value * damping * (
        curve_inner - 2.0 * tangent * slope_inner * slope_inner
    )
    return (activated, slope, bend)


def dot_nt(left, right):
    return lax.dot_general(left, right, (((1,), (1,)), ((), ())), preferred_element_type=F32)


def dot_tn(left, right):
    return lax.dot_general(left, right, (((0,), (0,)), ((), ())), preferred_element_type=F32)


def dot_nn(left, right):
    return jnp.dot(left, right, preferred_element_type=F32)


FORWARD_UNITS = 320
TILT_UNITS = 320
SPREAD_COLS = 512
BASE_UNITS = 160
TANGENT_UNITS = 320
UPDATE_UNITS = 320
FORWARD_LIMIT = 48
BASE_LIMIT = 50
TANGENT_LIMIT = 50
UPDATE_LIMIT = 58


def unit_block(units, wanted):
    return wanted if units % wanted == 0 else units


def whole(shape):
    zeros = (0,) * len(shape)
    return pl.BlockSpec(shape, lambda *_: zeros, pipeline_mode=pl.Buffered(1))


def call(body, grid, in_specs, out_specs, out_shape, scratch, flops, traffic, limit, args):
    return pl.pallas_call(
        body,
        grid=grid,
        in_specs=in_specs,
        out_specs=out_specs,
        out_shape=out_shape,
        scratch_shapes=scratch,
        compiler_params=pltpu.CompilerParams(
            dimension_semantics=("arbitrary",) * len(grid), vmem_limit_bytes=limit * 1024 * 1024
        ),
        cost_estimate=pl.CostEstimate(flops=flops, bytes_accessed=traffic, transcendentals=0),
    )(*args)


def column_sums(values, kind, out):
    rows, width = values.shape
    lanes = lax.broadcasted_iota(jnp.int32, (rows, 128), 1)
    cols = width // BLOCK_COLS
    for at in range(cols):
        part = values[:, at * BLOCK_COLS : (at + 1) * BLOCK_COLS]
        out = jnp.where(lanes == kind * cols + at, jnp.sum(part, axis=1, keepdims=True), out)
    return out


def norm_kernel(tokens, gain, out):
    x = tokens[...].astype(F32)
    factor = lax.rsqrt(jnp.mean(x * x, axis=-1, keepdims=True) + 1e-06)
    out[...] = (x * factor * gain[...]).astype(BF16)


def norm(tokens, gain):
    rows, width = tokens.shape
    return call(
        norm_kernel,
        (1,),
        [whole((rows, width)), whole((1, width))],
        whole((rows, width)),
        jax.ShapeDtypeStruct((rows, width), BF16),
        [],
        rows * width * 4,
        rows * width * 4,
        8,
        (tokens, gain.reshape(1, width)),
    )


def joined(refs):
    return jnp.concatenate([ref[...] for ref in refs], axis=1)


def forward_kernel(pieces, refs):
    blocks = refs[:pieces]
    (w, x, p_out, g_out, s_out, b_out, hid_out, own_q, sib_q, acc_q) = refs[pieces:]
    step = pl.program_id(0)
    rows = blocks[0].shape[0]

    @pl.when(step == 0)
    def _():
        for at in range(pieces):
            x[at * rows : (at + 1) * rows] = blocks[at][...]

    units, width = w.shape[1:]
    pre = dot_nt(w[0:2].reshape(2 * units, width), x[...])
    pre_gate, pre_up = (pre[:units], pre[units:])
    activated, slope, bend = gelu_parts(pre_gate)
    p_out[...] = pre_up * slope
    g_out[...] = activated
    s_out[...] = slope
    b_out[...] = pre_up * bend
    hidden = (activated * pre_up).astype(BF16)
    hid_out[...] = hidden
    quarter = acc_q.shape[1]
    first = pl.multiple_of(lax.axis_index("probe") * quarter, quarter)
    add_q = dot_tn(hidden, w[2, :, pl.ds(first, quarter)])

    @pl.when(step == 0)
    def _():
        acc_q[...] = add_q

    @pl.when(step > 0)
    def _():
        acc_q[...] += add_q

    @pl.when(step == pl.num_programs(0) - 1)
    def _():
        half = own_q.shape[0]
        own_q[...] = acc_q[:half]
        sib_q[...] = acc_q[half:].astype(sib_q.dtype)


def forward(blocks, weights, quarter, sib_type):
    rows, width = blocks[0].shape
    count = rows * len(blocks)
    kinds, units, _ = weights.shape
    ub = unit_block(units, FORWARD_UNITS)
    half = count // 2
    unit_spec = pl.BlockSpec((ub, count), lambda i: (i, 0))
    shape = jax.ShapeDtypeStruct
    return call(
        lambda *refs: forward_kernel(len(blocks), refs),
        (units // ub,),
        [whole((rows, width))] * len(blocks)
        + [pl.BlockSpec((kinds, ub, width), lambda i: (0, i, 0))],
        [whole((count, width))] + [unit_spec] * 5 + [whole((half, quarter))] * 2,
        [shape((count, width), BF16)]
        + [shape((units, count), F32)] * 4
        + [
            shape((units, count), BF16),
            shape((half, quarter), F32),
            shape((half, quarter), sib_type),
        ],
        [pltpu.VMEM((count, quarter), F32)],
        2 * count * units * width * 2,
        units * width * 6 + units * count * 18 + count * width * 4,
        FORWARD_LIMIT,
        (*blocks, weights),
    )


def tilt_kernel(z, x, p, g, s, b, q_out, s_out, tan_out):
    units, width = z.shape[2:]
    tan = dot_nt(z[0].reshape(2 * units, width), x[...])
    tan_gate, tan_up = (tan[:units], tan[units:])
    slope = s[...]
    q_out[...] = tan_up * slope + b[...] * tan_gate
    s_out[...] = slope * tan_gate
    tan_out[...] = (p[...] * tan_gate + g[...] * tan_up).astype(BF16)


def tilt(signs, x, p, g, s, b):
    count, width = x.shape
    units = p.shape[0]
    ub = unit_block(units, TILT_UNITS)
    unit_spec = pl.BlockSpec((ub, count), lambda i: (i, 0))
    shape = jax.ShapeDtypeStruct
    return call(
        tilt_kernel,
        (units // ub,),
        [pl.BlockSpec((1, 2, ub, width), lambda i: (0, 0, i, 0)), whole((count, width))]
        + [unit_spec] * 4,
        [unit_spec] * 3,
        [shape((units, count), F32)] * 2 + [shape((units, count), BF16)],
        [],
        2 * count * units * width * 2,
        units * width * 4 + units * count * 26 + count * width * 2,
        FORWARD_LIMIT,
        (signs, x, p, g, s, b),
    )


def spread_kernel(parts, refs):
    (w, z) = refs[:2]
    tans = refs[2 : 2 + parts]
    hids = refs[2 + parts : 2 + 2 * parts]
    (own, sib, left) = refs[2 + 2 * parts :]
    units, count = hids[0].shape

    @pl.when(pl.program_id(0) == 0)
    def _():
        for at in range(parts):
            span = slice(at * count, (at + 1) * count)
            left[span, :units] = tans[at][...].T
            left[span, units:] = hids[at][...].T

    total = dot_nn(left[...], jnp.concatenate([w[0], z[0, 0]], axis=0))
    half = count // 2
    for at in range(parts):
        base_row = at * count
        own[at * half : (at + 1) * half] = total[base_row : base_row + half]
        sib[at * half : (at + 1) * half] = total[base_row + half : base_row + count].astype(
            sib.dtype
        )


def spread(weights, signs, tans, hids, sib_type):
    units, count = hids[0].shape
    parts = len(hids)
    width = weights.shape[2]
    half = parts * count // 2
    cols = SPREAD_COLS
    shape = jax.ShapeDtypeStruct
    out_spec = pl.BlockSpec((half, cols), lambda i: (0, i))
    return call(
        lambda *refs: spread_kernel(parts, refs),
        (width // cols,),
        [
            pl.BlockSpec((1, units, cols), lambda i: (2, 0, i)),
            pl.BlockSpec((1, 1, units, cols), lambda i: (0, 2, 0, i)),
        ]
        + [whole((units, count))] * (2 * parts),
        [out_spec, out_spec],
        [shape((half, width), F32), shape((half, width), sib_type)],
        [pltpu.VMEM((parts * count, 2 * units), BF16)],
        4 * parts * count * units * width,
        units * width * 4 + half * width * 6,
        FORWARD_LIMIT,
        (weights, signs, *tans, *hids),
    )


def base_kernel(pieces, parts, refs):
    blocks = refs[: 2 * pieces]
    refs = refs[2 * pieces :]
    (w, z, m) = refs[:3]
    groups = [refs[3 + at * parts : 3 + (at + 1) * parts] for at in range(7)]
    (xs, ps, gs, qs, ss, hids, tans) = groups
    (new_m, e_gate, e_up, sums, normed, dout) = refs[3 + 7 * parts :]
    step = pl.program_id(0)
    half, quarter = blocks[0].shape
    chunk = 2 * half // parts

    @pl.when(step == 0)
    def _():
        me = lax.axis_index("probe")
        for at in range(pieces):
            first = pl.multiple_of((me ^ at) * quarter, quarter)
            for side in range(2):
                source = blocks[side * pieces + at]
                for part in range(parts):
                    start = part * chunk + side * (chunk // 2)
                    dout[start : start + chunk // 2, pl.ds(first, quarter)] = source[
                        part * (chunk // 2) : (part + 1) * (chunk // 2)
                    ]
        for part in range(parts):
            normed[part * chunk : (part + 1) * chunk] = xs[part][...]

    units = m.shape[1]
    d = dout[...]
    both = dot_nt(jnp.concatenate([w[0], z[0, 0]], axis=0), d)
    dhid, sdhid = (both[:units], both[units:])
    pv, gv = (joined(ps), joined(gs))
    e_gate[...] = sdhid * pv + dhid * joined(qs)
    e_up[...] = sdhid * gv + dhid * joined(ss)
    inner = jnp.concatenate([(dhid * pv).astype(BF16), (dhid * gv).astype(BF16)], axis=0)
    grads = dot_nn(inner, normed[...])
    new_m[0] = beta_one * m[0] + (1.0 - beta_one) * grads[:units]
    new_m[1] = beta_one * m[1] + (1.0 - beta_one) * grads[units:]
    outer = dot_nn(jnp.concatenate([joined(hids), joined(tans)], axis=0), d)
    new_m[2] = beta_one * m[2] + (1.0 - beta_one) * outer[:units]
    sums[...] = column_sums(z[0, 0].astype(F32) * outer[units:], 2, jnp.zeros((units, 128), F32))


def base(pieces, weights, signs, m, xs, ps, gs, qs, ss, hids, tans):
    half, quarter = pieces[0].shape
    kinds, units, width = weights.shape
    count = 2 * half
    parts = len(xs)
    chunk = count // parts
    ub = unit_block(units, BASE_UNITS)
    unit_spec = pl.BlockSpec((ub, count), lambda i: (i, 0))
    chunk_spec = pl.BlockSpec((ub, chunk), lambda i: (i, 0))
    mat_spec = pl.BlockSpec((kinds, ub, width), lambda i: (0, i, 0))
    sum_spec = pl.BlockSpec((ub, 128), lambda i: (i, 0))
    shape = jax.ShapeDtypeStruct
    return call(
        lambda *refs: base_kernel(len(pieces) // 2, parts, refs),
        (units // ub,),
        [whole((half, quarter))] * len(pieces)
        + [
            pl.BlockSpec((1, ub, width), lambda i: (2, i, 0)),
            pl.BlockSpec((1, 1, ub, width), lambda i: (0, 2, i, 0)),
            mat_spec,
        ]
        + [whole((chunk, width))] * parts
        + [chunk_spec] * (6 * parts),
        [mat_spec, unit_spec, unit_spec, sum_spec, whole((count, width))],
        [
            shape((kinds, units, width), F32),
            shape((units, count), F32),
            shape((units, count), F32),
            shape((units, 128), F32),
            shape((count, width), BF16),
        ],
        [pltpu.VMEM((count, width), BF16)],
        2 * count * units * width * 6,
        units * width * 28 + units * count * 28,
        BASE_LIMIT,
        (*pieces, weights, signs, m, *xs, *ps, *gs, *qs, *ss, *hids, *tans),
    )


def tangent_kernel(pieces, parts, refs):
    blocks = refs[:pieces]
    (w, z, normed, e_gate, e_up, sums_in) = refs[pieces : pieces + 6]
    refs = refs[pieces + 6 :]
    (ps, gs, hids) = [refs[at * parts : (at + 1) * parts] for at in range(3)]
    (sums, tdout, rows_sum, pairs) = refs[3 * parts :]
    step = pl.program_id(0)
    rows = blocks[0].shape[0]

    @pl.when(step == 0)
    def _():
        for at in range(pieces):
            tdout[at * rows : (at + 1) * rows] = blocks[at][...]

    units = e_gate.shape[0]
    t = tdout[...]
    tdh = dot_nt(w[0], t)
    inner = jnp.concatenate(
        [
            (tdh * joined(ps) + e_gate[...]).astype(BF16),
            (tdh * joined(gs) + e_up[...]).astype(BF16),
        ],
        axis=0,
    )
    hv = dot_nn(inner, normed[...])
    hv_out = dot_nn(joined(hids), t)
    made = jnp.zeros((units, 128), F32)
    made = column_sums(z[0, 0].astype(F32) * hv[:units], 0, made)
    made = column_sums(z[0, 1].astype(F32) * hv[units:], 1, made)
    made = column_sums(z[0, 2].astype(F32) * hv_out, 2, made)
    rows_sum[...] = made + sums_in[...]
    half = units // BLOCK_ROWS
    pairs[pl.ds(pl.multiple_of(step * half, 8), half), :] = (
        rows_sum[pl.ds(0, half, stride=2), :] + rows_sum[pl.ds(1, half, stride=2), :]
    )

    @pl.when(step == pl.num_programs(0) - 1)
    def _():
        sums[...] = pairs[...].T[: sums.shape[0]]


def tangent(blocks, weights, signs, normed, e_gate, e_up, sums, ps, gs, hids):
    rows, width = blocks[0].shape
    count = normed.shape[0]
    kinds, units, _ = weights.shape
    parts = len(ps)
    ub = unit_block(units, TANGENT_UNITS)
    unit_spec = pl.BlockSpec((ub, count), lambda i: (i, 0))
    chunk_spec = pl.BlockSpec((ub, count // parts), lambda i: (i, 0))
    cols = width // BLOCK_COLS
    return call(
        lambda *refs: tangent_kernel(len(blocks), parts, refs),
        (units // ub,),
        [whole((rows, width))] * len(blocks)
        + [
            pl.BlockSpec((1, ub, width), lambda i: (2, i, 0)),
            pl.BlockSpec((1, kinds, ub, width), lambda i: (0, 0, i, 0)),
            whole((count, width)),
            unit_spec,
            unit_spec,
            pl.BlockSpec((ub, 128), lambda i: (i, 0)),
        ]
        + [chunk_spec] * (3 * parts),
        whole((kinds * cols, units // BLOCK_ROWS)),
        jax.ShapeDtypeStruct((kinds * cols, units // BLOCK_ROWS), F32),
        [
            pltpu.VMEM((count, width), BF16),
            pltpu.VMEM((ub, 128), F32),
            pltpu.VMEM((units // BLOCK_ROWS, 128), F32),
        ],
        2 * count * units * width * 4,
        units * width * 8 + units * count * 18,
        TANGENT_LIMIT,
        (*blocks, weights, signs, normed, e_gate, e_up, sums, *ps, *gs, *hids),
    )


def update_kernel(probes, a, b, c, d, v, m, hess, new_v, update, scales):
    kinds, cols, half = v.shape
    kind, step = (pl.program_id(0), pl.program_id(1))

    @pl.when((kind == 0) & (step == 0))
    def _():
        total = (a[...] + b[...]) + (c[...] + d[...])
        for at in range(kinds):
            h = total[at * cols : (at + 1) * cols] * (1.0 / (BLOCK_ROWS * BLOCK_COLS * probes))
            hess[at] = h
            nv = beta_two * v[at] + (1.0 - beta_two) * h * h
            new_v[at] = nv
            denom = jnp.sqrt(nv / (1.0 - beta_two**STEP)) + epsilon
            scale = 1.0 / (denom * (1.0 - beta_one**STEP))
            wide = jnp.concatenate([scale, jnp.zeros((128 - cols, half), F32)], axis=0).T
            scales[at, pl.ds(0, half, stride=2), :] = wide
            scales[at, pl.ds(1, half, stride=2), :] = wide

    tall = m.shape[1]
    full = scales[kind, pl.ds(pl.multiple_of(step * tall, tall), tall), :]
    for at in range(cols):
        span = slice(at * BLOCK_COLS, (at + 1) * BLOCK_COLS)
        update[0, :, span] = m[0, :, span] * full[:, at : at + 1]


def update_step(sums, v, m):
    kinds, units, width = m.shape
    ub = unit_block(units, UPDATE_UNITS)
    m_spec = pl.BlockSpec((1, ub, width), lambda k, i: (k, i, 0))
    shape = jax.ShapeDtypeStruct
    return call(
        functools.partial(update_kernel, len(sums)),
        (kinds, units // ub),
        [whole(sums[0].shape)] * 4 + [whole(v.shape), m_spec],
        [whole(v.shape), whole(v.shape), m_spec],
        [shape(v.shape, F32), shape(v.shape, F32), shape(m.shape, F32)],
        [pltpu.VMEM((kinds, units, 128), F32)],
        units * width * 6,
        units * width * 24,
        UPDATE_LIMIT,
        (*sums, v, m),
    )


def to_sibling(x, chips):
    return lax.ppermute(x, "mp", [(i, i ^ 1) for i in range(2 * chips)])


def to_chip(x, chips, flip):
    pairs = [(2 * z + c, 2 * (z ^ flip) + c) for z in range(chips) for c in range(2)]
    return lax.ppermute(x, "mp", pairs)


def to_probe(x, probes, flip):
    return lax.ppermute(x, "probe", [(i, i ^ flip) for i in range(probes)])


def gather_rows(x, chips):
    own = [x]
    for flip in range(1, chips):
        own.append(to_chip(x, chips, flip))
    sib = []
    for flip in range(chips):
        sib.append(to_sibling(own[flip], chips))
    half = chips // 2
    return [own[:half] + sib[:half], own[half:] + sib[half:]]


def near_path(normed, offset, weights, probe_signs, m_state, chips, probes):
    rows, width = normed.shape
    count = 2 * chips * rows
    quarter = width // probes
    chunks = gather_rows(normed, chips)
    xs, ps, gs, qs, ss, hids, tans, totals = ([], [], [], [], [], [], [], [])
    for blocks in chunks:
        x, p, g, s, b, hid, own_q, sib_q = forward(blocks, weights, quarter, BF16)
        got = to_sibling(sib_q, chips)
        totals.append(own_q + got.astype(F32))
        q, s, tan = tilt(probe_signs, x, p, g, s, b)
        for held, value in zip((xs, ps, gs, qs, ss, hids, tans), (x, p, g, q, s, hid, tan)):
            held.append(value)
    own_t, sib_t = spread(weights, probe_signs, tans, hids, BF16)
    kept = totals[0][:rows] + offset
    for flip in range(1, chips):
        part = totals[flip // 2][(flip % 2) * rows : (flip % 2 + 1) * rows].astype(BF16)
        kept = kept + to_chip(part, chips, flip).astype(F32)
    part = (kept / count).astype(BF16)
    mine = [part]
    for flip in range(1, chips):
        mine.append(to_chip(part, chips, flip))
    mine = jnp.concatenate(mine, axis=0)
    pieces = [mine]
    for flip in range(1, probes):
        pieces.append(to_probe(mine, probes, flip))
    for at in range(probes):
        pieces.append(to_sibling(pieces[at], chips))
    got = to_sibling(sib_t, chips)
    total = own_t + got.astype(F32)
    kept = total[:rows]
    for flip in range(1, chips):
        part = total[flip * rows : (flip + 1) * rows].astype(BF16)
        kept = kept + to_chip(part, chips, flip).astype(F32)
    tan_dout = (kept / count).astype(BF16)
    tan_blocks = gather_rows(tan_dout, chips)
    new_m, e_gate, e_up, sums, full = base(
        pieces, weights, probe_signs, m_state, xs, ps, gs, qs, ss, hids, tans
    )
    sums = tangent(
        tan_blocks[0] + tan_blocks[1],
        weights,
        probe_signs,
        full,
        e_gate,
        e_up,
        sums,
        ps,
        gs,
        hids,
    )
    return new_m, sums


def far_path(normed, offset, weights, probe_signs, m_state, chips, probes):
    rows, width = normed.shape
    count = 2 * chips * rows
    quarter = width // probes
    blocks = [lax.all_gather(normed, "mp", axis=0, tiled=True)]
    x, p, g, s, b, hid, own_q, sib_q = forward(blocks, weights, quarter, F32)
    q, s, tan = tilt(probe_signs, x, p, g, s, b)
    own_t, sib_t = spread(weights, probe_signs, [tan], [hid], F32)
    part = lax.psum_scatter(
        jnp.concatenate([own_q, sib_q], axis=0), "mp", scatter_dimension=0, tiled=True
    )
    mine = lax.all_gather(
        ((part + offset) / count).astype(BF16), "mp", axis=0, tiled=True
    )
    pieces = [mine] + [to_probe(mine, probes, flip) for flip in range(1, probes)]
    half = count // 2
    pieces = [piece[:half] for piece in pieces] + [piece[half:] for piece in pieces]
    kept = lax.psum_scatter(
        jnp.concatenate([own_t, sib_t], axis=0), "mp", scatter_dimension=0, tiled=True
    )
    tan_blocks = [lax.all_gather((kept / count).astype(BF16), "mp", axis=0, tiled=True)]
    new_m, e_gate, e_up, sums, full = base(
        pieces, weights, probe_signs, m_state, [x], [p], [g], [q], [s], [hid], [tan]
    )
    sums = tangent(
        tan_blocks, weights, probe_signs, full, e_gate, e_up, sums, [p], [g], [hid]
    )
    return new_m, sums


def shards(tokens, targets, norm_gain, weights, probe_signs, m_state, v_state):
    probes = lax.axis_size("probe")
    chips = lax.axis_size("mp") // 2
    quarter = tokens.shape[1] // probes
    first = lax.axis_index("probe") * quarter
    normed = norm(tokens, norm_gain)
    offset = lax.dynamic_slice_in_dim(tokens, first, quarter, 1).astype(
        F32
    ) - lax.dynamic_slice_in_dim(targets, first, quarter, 1).astype(F32)
    path = near_path if chips == 4 else far_path
    new_m, sums = path(normed, offset, weights, probe_signs, m_state, chips, probes)
    sums = [sums] + [to_probe(sums, probes, flip) for flip in range(1, probes)]
    hess, new_v, update = update_step(sums, v_state.transpose(0, 2, 1), new_m)
    return (hess.transpose(0, 2, 1), new_m, new_v.transpose(0, 2, 1), update)


def solution(mesh):
    return jax.shard_map(
        shards,
        mesh=mesh,
        in_specs=(
            P("mp", None),
            P("mp", None),
            P(),
            P(None, "mp", None),
            P("probe", None, "mp", None),
            P(None, "mp", None),
            P(None, "mp", None),
        ),
        out_specs=(
            P(None, "mp", None),
            P(None, "mp", None),
            P(None, "mp", None),
            P(None, "mp", None),
        ),
        check_vma=False,
    )
```

```python
import functools
import math

import jax
import jax.numpy as jnp
from jax import lax
from jax.experimental import pallas as pl
from jax.experimental.pallas import tpu as pltpu
from jax.sharding import PartitionSpec as P


BLOCK_ROWS = 2
BLOCK_COLS = 128
STEP = 4

beta_one = 0.9
beta_two = 0.999
epsilon = 0.0001
root_half = 0.7978845608028654
cubic = 0.044715

F32 = jnp.float32
BF16 = jnp.bfloat16


def gelu_parts(value):
    square = value * value
    inner = root_half * (value + cubic * square * value)
    slope_inner = root_half * (1.0 + 3.0 * cubic * square)
    curve_inner = 6.0 * root_half * cubic * value
    tangent = jnp.tanh(inner)
    damping = 1.0 - tangent * tangent
    activated = 0.5 * value * (1.0 + tangent)
    slope = 0.5 * (1.0 + tangent) + 0.5 * value * damping * slope_inner
    bend = damping * slope_inner + 0.5 * value * damping * (
        curve_inner - 2.0 * tangent * slope_inner * slope_inner
    )
    return (activated, slope, bend)


def dot_nt(left, right):
    return lax.dot_general(left, right, (((1,), (1,)), ((), ())), preferred_element_type=F32)


def dot_tn(left, right):
    return lax.dot_general(left, right, (((0,), (0,)), ((), ())), preferred_element_type=F32)


def dot_nn(left, right):
    return jnp.dot(left, right, preferred_element_type=F32)


FORWARD_UNITS = 320
TILT_UNITS = 320
SPREAD_COLS = 512
BASE_UNITS = 160
TANGENT_UNITS = 320
UPDATE_UNITS = 320
FORWARD_LIMIT = 24
BASE_LIMIT = 28
TANGENT_LIMIT = 32
UPDATE_LIMIT = 16


def unit_block(units, wanted):
    return wanted if units % wanted == 0 else units


def whole(shape):
    zeros = (0,) * len(shape)
    return pl.BlockSpec(shape, lambda *_: zeros, pipeline_mode=pl.Buffered(1))


def in_vmem(array):
    return pltpu.with_memory_space_constraint(array, pltpu.VMEM)


def in_hbm(array):
    return pltpu.with_memory_space_constraint(array, pltpu.HBM)


HELD = pl.BlockSpec(memory_space=pltpu.VMEM)


def call(body, grid, in_specs, out_specs, out_shape, scratch, flops, traffic, limit, args, aliases={}):
    return pl.pallas_call(
        body,
        grid=grid,
        in_specs=in_specs,
        out_specs=out_specs,
        out_shape=out_shape,
        scratch_shapes=scratch,
        input_output_aliases=aliases,
        compiler_params=pltpu.CompilerParams(
            dimension_semantics=("arbitrary",) * len(grid), vmem_limit_bytes=limit * 1024 * 1024
        ),
        cost_estimate=pl.CostEstimate(flops=flops, bytes_accessed=traffic, transcendentals=0),
    )(*args)


def column_sums(values, kind, out):
    rows, width = values.shape
    lanes = lax.broadcasted_iota(jnp.int32, (rows, 128), 1)
    cols = width // BLOCK_COLS
    for at in range(cols):
        part = values[:, at * BLOCK_COLS : (at + 1) * BLOCK_COLS]
        out = jnp.where(lanes == kind * cols + at, jnp.sum(part, axis=1, keepdims=True), out)
    return out


def norm_kernel(tokens, gain, out):
    x = tokens[...].astype(F32)
    factor = lax.rsqrt(jnp.mean(x * x, axis=-1, keepdims=True) + 1e-06)
    out[...] = (x * factor * gain[...]).astype(BF16)


def norm(tokens, gain):
    rows, width = tokens.shape
    return call(
        norm_kernel,
        (1,),
        [whole((rows, width)), whole((1, width))],
        whole((rows, width)),
        jax.ShapeDtypeStruct((rows, width), BF16),
        [],
        rows * width * 4,
        rows * width * 4,
        8,
        (in_hbm(tokens), in_hbm(gain.reshape(1, width))),
    )


def joined(refs):
    return jnp.concatenate([ref[...] for ref in refs], axis=1)


def forward_kernel(pieces, chunk, refs):
    blocks = refs[:pieces]
    w = refs[pieces]
    (x, p_out, g_out, s_out, b_out, hid_out, own_q, sib_q, acc_q) = refs[-9:]
    step = pl.program_id(0)
    rows = blocks[0].shape[0]
    count = rows * pieces
    first_row = chunk * count

    @pl.when(step == 0)
    def _():
        for at in range(pieces):
            x[first_row + at * rows : first_row + (at + 1) * rows] = blocks[at][...]

    total, width = w.shape[1:]
    units = unit_block(total, FORWARD_UNITS)
    span = pl.ds(pl.multiple_of(step * units, 16), units)
    pre = dot_nt(w[0:2, span].reshape(2 * units, width), x[first_row : first_row + count])
    pre_gate, pre_up = (pre[:units], pre[units:])
    activated, slope, bend = gelu_parts(pre_gate)
    p_out[span] = pre_up * slope
    g_out[span] = activated
    s_out[span] = slope
    b_out[span] = pre_up * bend
    hidden = (activated * pre_up).astype(BF16)
    hid_out[span] = hidden
    quarter = acc_q.shape[1]
    first = pl.multiple_of(lax.axis_index("probe") * quarter, quarter)
    add_q = dot_tn(hidden, w[2, span, pl.ds(first, quarter)])

    @pl.when(step == 0)
    def _():
        acc_q[...] = add_q

    @pl.when(step > 0)
    def _():
        acc_q[...] += add_q

    @pl.when(step == pl.num_programs(0) - 1)
    def _():
        half = own_q.shape[0]
        own_q[...] = acc_q[:half]
        sib_q[...] = acc_q[half:].astype(sib_q.dtype)


def forward(blocks, weights, chunk, chunks, x, quarter, sib_type):
    rows, width = blocks[0].shape
    count = rows * len(blocks)
    units = weights.shape[1]
    ub = unit_block(units, FORWARD_UNITS)
    half = count // 2
    held = [] if x is None else [x]
    return call(
        lambda *refs: forward_kernel(len(blocks), chunk, refs),
        (units // ub,),
        [whole((rows, width))] * len(blocks) + [HELD] * (1 + len(held)),
        [HELD] * 8,
        [pltpu.VMEM((count * chunks, width), BF16)]
        + [pltpu.VMEM((units, count), F32)] * 4
        + [
            pltpu.VMEM((units, count), BF16),
            pltpu.VMEM((half, quarter), F32),
            pltpu.VMEM((half, quarter), sib_type),
        ],
        [pltpu.VMEM((count, quarter), F32)],
        2 * count * units * width * 2,
        units * width * 6 + units * count * 18 + count * width * 4,
        FORWARD_LIMIT,
        (*blocks, in_vmem(weights), *map(in_vmem, held)),
        {len(blocks) + 1: 0} if held else {},
    )


def tilt_kernel(chunk, z, x, p, g, s, b, q_out, s_out, tan_out):
    total, width = z.shape[1:]
    units = unit_block(total, TILT_UNITS)
    count = p.shape[1]
    span = pl.ds(pl.multiple_of(pl.program_id(0) * units, 16), units)
    rows = slice(chunk * count, (chunk + 1) * count)
    tan = dot_nt(z[0:2, span].reshape(2 * units, width), x[rows])
    tan_gate, tan_up = (tan[:units], tan[units:])
    slope = s[span]
    q_out[span] = tan_up * slope + b[span] * tan_gate
    s_out[span] = slope * tan_gate
    tan_out[span] = (p[span] * tan_gate + g[span] * tan_up).astype(BF16)


def tilt(signs, chunk, x, p, g, s, b):
    units, count = p.shape
    width = x.shape[1]
    ub = unit_block(units, TILT_UNITS)
    return call(
        functools.partial(tilt_kernel, chunk),
        (units // ub,),
        [HELD] * 6,
        [HELD] * 3,
        [pltpu.VMEM((units, count), F32)] * 2 + [pltpu.VMEM((units, count), BF16)],
        [],
        2 * count * units * width * 2,
        units * width * 4 + units * count * 26 + count * width * 2,
        FORWARD_LIMIT,
        tuple(map(in_vmem, (signs, x, p, g, s, b))),
    )


def spread_kernel(parts, refs):
    (w, z) = refs[:2]
    tans = refs[2 : 2 + parts]
    hids = refs[2 + parts : 2 + 2 * parts]
    (own, sib, left) = refs[2 + 2 * parts :]
    units, count = hids[0].shape
    step = pl.program_id(0)

    @pl.when(step == 0)
    def _():
        for at in range(parts):
            span = slice(at * count, (at + 1) * count)
            left[span, :units] = tans[at][...].T
            left[span, units:] = hids[at][...].T

    cols = min(SPREAD_COLS, own.shape[1])
    span = pl.ds(pl.multiple_of(step * cols, cols), cols)
    total = dot_nn(left[...], jnp.concatenate([w[2, :, span], z[2, :, span]], axis=0))
    half = count // 2
    for at in range(parts):
        top = at * count
        rows = slice(at * half, (at + 1) * half)
        own[rows, span] = total[top : top + half]
        sib[rows, span] = total[top + half : top + count].astype(sib.dtype)


def spread(weights, signs, tans, hids, sib_type):
    units, count = hids[0].shape
    parts = len(hids)
    width = weights.shape[2]
    half = parts * count // 2
    cols = SPREAD_COLS
    return call(
        lambda *refs: spread_kernel(parts, refs),
        (width // cols,),
        [HELD] * (2 + 2 * parts),
        [HELD, HELD],
        [pltpu.VMEM((half, width), F32), pltpu.VMEM((half, width), sib_type)],
        [pltpu.VMEM((parts * count, 2 * units), BF16)],
        4 * parts * count * units * width,
        units * width * 4 + half * width * 6,
        FORWARD_LIMIT,
        tuple(map(in_vmem, (weights, signs, *tans, *hids))),
    )


def fold_kernel(parts, rows, refs):
    owns = refs[:parts]
    gots = refs[parts : 2 * parts]
    outs = refs[2 * parts :]
    at = 0
    for own, got in zip(owns, gots):
        for first in range(0, own.shape[0], rows):
            span = slice(first, first + rows)
            outs[at][...] = (own[span] + got[span].astype(F32)).astype(outs[at].dtype)
            at += 1


def fold(owns, gots, rows):
    parts = len(owns)
    blocks = sum(own.shape[0] for own in owns) // rows
    width = owns[0].shape[1]
    return call(
        lambda *refs: fold_kernel(parts, rows, refs),
        (1,),
        [HELD] * (2 * parts),
        [HELD] * blocks,
        [pltpu.VMEM((rows, width), F32)] + [pltpu.VMEM((rows, width), BF16)] * (blocks - 1),
        [],
        rows * blocks * width * 64,
        rows * blocks * width * 8,
        8,
        tuple(map(in_vmem, (*owns, *gots))),
    )


def load_kernel(plan, refs):
    count = len(plan)
    (sources, targets, sems) = (refs[:count], refs[count : 2 * count], refs[2 * count])
    copies = []
    for source, target, picks in zip(sources, targets, plan):
        for place, pick in enumerate(picks):
            copies.append(
                pltpu.make_async_copy(source.at[pick], target.at[place], sems.at[len(copies)])
            )
    for copy in copies:
        copy.start()
    for copy in copies:
        copy.wait()


def load(arrays, plan):
    shapes = [(len(picks), *array.shape[1:]) for array, picks in zip(arrays, plan)]
    size = sum(math.prod(dims) for dims in shapes)
    return pl.pallas_call(
        lambda *refs: load_kernel(plan, refs),
        name="load",
        in_specs=[pl.BlockSpec(memory_space=pltpu.HBM)] * len(arrays),
        out_specs=[HELD] * len(arrays),
        out_shape=[pltpu.VMEM(dims, array.dtype) for dims, array in zip(shapes, arrays)],
        scratch_shapes=[pltpu.SemaphoreType.DMA((sum(map(len, plan)),))],
        compiler_params=pltpu.CompilerParams(vmem_limit_bytes=8 * 1024 * 1024),
        cost_estimate=pl.CostEstimate(
            flops=size * 64, bytes_accessed=size * 8, transcendentals=0
        ),
    )(*map(in_hbm, arrays))


def load_moment(array):
    kinds, units, width = array.shape
    ub = unit_block(units, BASE_UNITS)
    split = array.reshape(kinds * units // ub, ub, width)
    return load([split], [tuple(range(split.shape[0]))])[0]


def load_weights(weights, signs):
    kinds, units, width = weights.shape
    halves = 2 if units % 32 == 0 else 1
    dims = (kinds * halves, units // halves, width)
    picks = tuple(range(kinds * halves))
    loaded = load([weights.reshape(dims), signs.reshape(dims)], [picks, picks])
    return [array.reshape(kinds, units, width) for array in loaded]


def joined(refs, span):
    return jnp.concatenate([ref[span] for ref in refs], axis=1)


def base_kernel(pieces, parts, refs):
    blocks = refs[: 2 * pieces]
    refs = refs[2 * pieces :]
    (w, z, m, normed) = refs[:4]
    groups = [refs[4 + at * parts : 4 + (at + 1) * parts] for at in range(6)]
    (ps, gs, qs, ss, hids, tans) = groups
    (new_m, held, e_gate, e_up, sums, dout) = refs[4 + 6 * parts :]
    step = pl.program_id(0)
    half, quarter = blocks[0].shape
    chunk = 2 * half // parts

    @pl.when(step == 0)
    def _():
        me = lax.axis_index("probe")
        for at in range(pieces):
            first = pl.multiple_of((me ^ at) * quarter, quarter)
            for side in range(2):
                source = blocks[side * pieces + at]
                for part in range(parts):
                    start = part * chunk + side * (chunk // 2)
                    dout[start : start + chunk // 2, pl.ds(first, quarter)] = source[
                        part * (chunk // 2) : (part + 1) * (chunk // 2)
                    ]

    units = w.shape[1]
    kinds = new_m.shape[0]
    blocks_of = m.shape[0] // kinds
    span = pl.ds(pl.multiple_of(step * units, 16), units)
    d = dout[...]
    both = dot_nt(jnp.concatenate([w[0], z[0, 0]], axis=0), d)
    dhid, sdhid = (both[:units], both[units:])
    pv, gv = (joined(ps, span), joined(gs, span))
    e_gate[span] = sdhid * pv + dhid * joined(qs, span)
    e_up[span] = sdhid * gv + dhid * joined(ss, span)
    inner = jnp.concatenate([(dhid * pv).astype(BF16), (dhid * gv).astype(BF16)], axis=0)
    grads = dot_nn(inner, normed[...])

    def moment(kind, grad):
        at = kind * blocks_of + step
        value = beta_one * m[at] + (1.0 - beta_one) * grad
        new_m[kind] = value
        held[at] = value

    moment(0, grads[:units])
    moment(1, grads[units:])
    outer = dot_nn(jnp.concatenate([joined(hids, span), joined(tans, span)], axis=0), d)
    moment(2, outer[:units])
    sums[span] = column_sums(z[0, 0].astype(F32) * outer[units:], 2, jnp.zeros((units, 128), F32))


def base(pieces, weights, signs, m, x, ps, gs, qs, ss, hids, tans):
    half, quarter = pieces[0].shape
    kinds, units, width = weights.shape
    count = 2 * half
    parts = len(ps)
    ub = unit_block(units, BASE_UNITS)
    return call(
        lambda *refs: base_kernel(len(pieces) // 2, parts, refs),
        (units // ub,),
        [whole((half, quarter))] * len(pieces)
        + [
            pl.BlockSpec((1, ub, width), lambda i: (2, i, 0)),
            pl.BlockSpec((1, 1, ub, width), lambda i: (0, 2, i, 0)),
        ]
        + [HELD] * (2 + 6 * parts),
        [pl.BlockSpec((kinds, ub, width), lambda i: (0, i, 0))] + [HELD] * 4,
        [
            jax.ShapeDtypeStruct((kinds, units, width), F32),
            pltpu.VMEM(m.shape, F32),
            pltpu.VMEM((units, count), F32),
            pltpu.VMEM((units, count), F32),
            pltpu.VMEM((units, 128), F32),
        ],
        [pltpu.VMEM((count, width), BF16)],
        2 * count * units * width * 6,
        units * width * 28 + units * count * 28,
        BASE_LIMIT,
        (
            *pieces,
            in_hbm(weights),
            in_hbm(signs),
            *map(in_vmem, (m, x, *ps, *gs, *qs, *ss, *hids, *tans)),
        ),
        {len(pieces) + 2: 1},
    )


def tangent_kernel(pieces, parts, refs):
    blocks = refs[:pieces]
    (w, z, normed, e_gate, e_up, sums_in) = refs[pieces : pieces + 6]
    refs = refs[pieces + 6 :]
    (ps, gs, hids) = [refs[at * parts : (at + 1) * parts] for at in range(3)]
    (sums, tdout, rows_sum, pairs) = refs[3 * parts :]
    step = pl.program_id(0)
    rows = blocks[0].shape[0]

    @pl.when(step == 0)
    def _():
        for at in range(pieces):
            tdout[at * rows : (at + 1) * rows] = blocks[at][...]

    units = w.shape[1]
    span = pl.ds(pl.multiple_of(step * units, 16), units)
    t = tdout[...]
    tdh = dot_nt(w[0], t)
    inner = jnp.concatenate(
        [
            (tdh * joined(ps, span) + e_gate[span]).astype(BF16),
            (tdh * joined(gs, span) + e_up[span]).astype(BF16),
        ],
        axis=0,
    )
    hv = dot_nn(inner, normed[...])
    hv_out = dot_nn(joined(hids, span), t)
    made = jnp.zeros((units, 128), F32)
    made = column_sums(z[0, 0].astype(F32) * hv[:units], 0, made)
    made = column_sums(z[0, 1].astype(F32) * hv[units:], 1, made)
    made = column_sums(z[0, 2].astype(F32) * hv_out, 2, made)
    rows_sum[...] = made + sums_in[span]
    half = units // BLOCK_ROWS
    pairs[pl.ds(pl.multiple_of(step * half, 8), half), :] = (
        rows_sum[pl.ds(0, half, stride=2), :] + rows_sum[pl.ds(1, half, stride=2), :]
    )

    @pl.when(step == pl.num_programs(0) - 1)
    def _():
        sums[...] = pairs[...].T[: sums.shape[0]]


def tangent(blocks, weights, signs, normed, e_gate, e_up, sums, ps, gs, hids):
    rows, width = blocks[0].shape
    count = normed.shape[0]
    kinds, units, _ = weights.shape
    parts = len(ps)
    ub = unit_block(units, TANGENT_UNITS)
    cols = width // BLOCK_COLS
    return call(
        lambda *refs: tangent_kernel(len(blocks), parts, refs),
        (units // ub,),
        [whole((rows, width))] * len(blocks)
        + [
            pl.BlockSpec((1, ub, width), lambda i: (2, i, 0)),
            pl.BlockSpec((1, kinds, ub, width), lambda i: (0, 0, i, 0)),
        ]
        + [HELD] * (4 + 3 * parts),
        whole((kinds * cols, units // BLOCK_ROWS)),
        jax.ShapeDtypeStruct((kinds * cols, units // BLOCK_ROWS), F32),
        [
            pltpu.VMEM((count, width), BF16),
            pltpu.VMEM((ub, 128), F32),
            pltpu.VMEM((units // BLOCK_ROWS, 128), F32),
        ],
        2 * count * units * width * 4,
        units * width * 8 + units * count * 18,
        TANGENT_LIMIT,
        (
            *blocks,
            in_hbm(weights),
            in_hbm(signs),
            *map(in_vmem, (normed, e_gate, e_up, sums, *ps, *gs, *hids)),
        ),
    )


def update_kernel(probes, a, b, c, d, v, m, hess, new_v, update, scales):
    kinds, cols, half = v.shape
    kind, step = (pl.program_id(0), pl.program_id(1))

    @pl.when((kind == 0) & (step == 0))
    def _():
        total = (a[...] + b[...]) + (c[...] + d[...])
        for at in range(kinds):
            h = total[at * cols : (at + 1) * cols] * (1.0 / (BLOCK_ROWS * BLOCK_COLS * probes))
            hess[at] = h
            nv = beta_two * v[at] + (1.0 - beta_two) * h * h
            new_v[at] = nv
            denom = jnp.sqrt(nv / (1.0 - beta_two**STEP)) + epsilon
            scale = 1.0 / (denom * (1.0 - beta_one**STEP))
            wide = jnp.concatenate([scale, jnp.zeros((128 - cols, half), F32)], axis=0).T
            scales[at, pl.ds(0, half, stride=2), :] = wide
            scales[at, pl.ds(1, half, stride=2), :] = wide

    tall = update.shape[1]
    full = scales[kind, pl.ds(pl.multiple_of(step * tall, tall), tall), :]
    pieces = tall // m.shape[1]
    first = (kind * pl.num_programs(1) + step) * pieces
    for piece in range(pieces):
        rows = slice(piece * m.shape[1], (piece + 1) * m.shape[1])
        for at in range(cols):
            span = slice(at * BLOCK_COLS, (at + 1) * BLOCK_COLS)
            update[0, rows, span] = m[first + piece, :, span] * full[rows, at : at + 1]


def update_step(sums, v, m):
    kinds, _, half = v.shape
    units, width = (half * BLOCK_ROWS, m.shape[2])
    ub = unit_block(units, UPDATE_UNITS)
    m_spec = pl.BlockSpec((1, ub, width), lambda k, i: (k, i, 0))
    shape = jax.ShapeDtypeStruct
    return call(
        functools.partial(update_kernel, len(sums)),
        (kinds, units // ub),
        [whole(sums[0].shape)] * 4 + [whole(v.shape), pl.BlockSpec(memory_space=pltpu.VMEM)],
        [whole(v.shape), whole(v.shape), m_spec],
        [shape(v.shape, F32), shape(v.shape, F32), shape((kinds, units, width), F32)],
        [pltpu.VMEM((kinds, units, 128), F32)],
        units * width * 6,
        units * width * 24,
        UPDATE_LIMIT,
        (*sums, v, in_vmem(m)),
    )


def to_sibling(x, chips):
    return lax.ppermute(x, "mp", [(i, i ^ 1) for i in range(2 * chips)])


def to_chip(x, chips, flip):
    pairs = [(2 * z + c, 2 * (z ^ flip) + c) for z in range(chips) for c in range(2)]
    return lax.ppermute(x, "mp", pairs)


def to_probe(x, probes, flip):
    return lax.ppermute(x, "probe", [(i, i ^ flip) for i in range(probes)])


def gather_rows(x, chips):
    own = [x]
    for flip in range(1, chips):
        own.append(to_chip(x, chips, flip))
    sib = []
    for flip in range(chips):
        sib.append(to_sibling(own[flip], chips))
    half = chips // 2
    return [own[:half] + sib[:half], own[half:] + sib[half:]]


def near_path(normed, offset, weights, probe_signs, m_state, chips, probes):
    rows, width = normed.shape
    count = 2 * chips * rows
    quarter = width // probes
    chunks = gather_rows(normed, chips)
    w, z = load_weights(weights, probe_signs)
    x = None
    ps, gs, qs, ss, hids, tans, owns, gots = ([], [], [], [], [], [], [], [])
    for at, blocks in enumerate(chunks):
        x, p, g, s, b, hid, own_q, sib_q = forward(
            blocks, w, at, len(chunks), x, quarter, BF16
        )
        gots.append(to_sibling(sib_q, chips))
        owns.append(own_q)
        q, s, tan = tilt(z, at, x, p, g, s, b)
        for held, value in zip((ps, gs, qs, ss, hids, tans), (p, g, q, s, hid, tan)):
            held.append(value)
    own_t, sib_t = spread(w, z, tans, hids, BF16)
    kept, *sent = fold(owns, gots, rows)
    kept = kept + offset
    for flip in range(1, chips):
        kept = kept + to_chip(sent[flip - 1], chips, flip).astype(F32)
    part = (kept / count).astype(BF16)
    mine = [part]
    for flip in range(1, chips):
        mine.append(to_chip(part, chips, flip))
    mine = jnp.concatenate(mine, axis=0)
    pieces = [mine]
    for flip in range(1, probes):
        pieces.append(to_probe(mine, probes, flip))
    for at in range(probes):
        pieces.append(to_sibling(pieces[at], chips))
    got = to_sibling(sib_t, chips)
    kept, *sent = fold([own_t], [got], rows)
    for flip in range(1, chips):
        kept = kept + to_chip(sent[flip - 1], chips, flip).astype(F32)
    tan_dout = (kept / count).astype(BF16)
    tan_blocks = gather_rows(tan_dout, chips)
    held = load_moment(m_state)
    new_m, held, e_gate, e_up, sums = base(
        pieces, weights, probe_signs, held, x, ps, gs, qs, ss, hids, tans
    )
    sums = tangent(
        tan_blocks[0] + tan_blocks[1],
        weights,
        probe_signs,
        x,
        e_gate,
        e_up,
        sums,
        ps,
        gs,
        hids,
    )
    return new_m, held, sums


def far_path(normed, offset, weights, probe_signs, m_state, chips, probes):
    rows, width = normed.shape
    count = 2 * chips * rows
    quarter = width // probes
    blocks = [lax.all_gather(normed, "mp", axis=0, tiled=True)]
    w, z = load_weights(weights, probe_signs)
    x, p, g, s, b, hid, own_q, sib_q = forward(blocks, w, 0, 1, None, quarter, F32)
    q, s, tan = tilt(z, 0, x, p, g, s, b)
    own_t, sib_t = spread(w, z, [tan], [hid], F32)
    part = lax.psum_scatter(
        jnp.concatenate([own_q, sib_q], axis=0), "mp", scatter_dimension=0, tiled=True
    )
    mine = lax.all_gather(
        ((part + offset) / count).astype(BF16), "mp", axis=0, tiled=True
    )
    pieces = [mine] + [to_probe(mine, probes, flip) for flip in range(1, probes)]
    half = count // 2
    pieces = [piece[:half] for piece in pieces] + [piece[half:] for piece in pieces]
    kept = lax.psum_scatter(
        jnp.concatenate([own_t, sib_t], axis=0), "mp", scatter_dimension=0, tiled=True
    )
    tan_blocks = [lax.all_gather((kept / count).astype(BF16), "mp", axis=0, tiled=True)]
    held = load_moment(m_state)
    new_m, held, e_gate, e_up, sums = base(
        pieces, weights, probe_signs, held, x, [p], [g], [q], [s], [hid], [tan]
    )
    sums = tangent(
        tan_blocks, weights, probe_signs, x, e_gate, e_up, sums, [p], [g], [hid]
    )
    return new_m, held, sums


def shards(tokens, targets, norm_gain, weights, probe_signs, m_state, v_state):
    probes = lax.axis_size("probe")
    chips = lax.axis_size("mp") // 2
    quarter = tokens.shape[1] // probes
    first = lax.axis_index("probe") * quarter
    normed = norm(tokens, norm_gain)
    offset = lax.dynamic_slice_in_dim(tokens, first, quarter, 1).astype(
        F32
    ) - lax.dynamic_slice_in_dim(targets, first, quarter, 1).astype(F32)
    path = near_path if chips == 4 else far_path
    new_m, held, sums = path(normed, offset, weights, probe_signs, m_state, chips, probes)
    sums = [sums] + [to_probe(sums, probes, flip) for flip in range(1, probes)]
    hess, new_v, update = update_step(sums, v_state.transpose(0, 2, 1), held)
    return (hess.transpose(0, 2, 1), new_m, new_v.transpose(0, 2, 1), update)


def solution(mesh):
    return jax.shard_map(
        shards,
        mesh=mesh,
        in_specs=(
            P("mp", None),
            P("mp", None),
            P(),
            P(None, "mp", None),
            P("probe", None, "mp", None),
            P(None, "mp", None),
            P(None, "mp", None),
        ),
        out_specs=(
            P(None, "mp", None),
            P(None, "mp", None),
            P(None, "mp", None),
            P(None, "mp", None),
        ),
        check_vma=False,
    )
```

```python
import functools
import math

import jax
import jax.numpy as jnp
from jax import lax
from jax.experimental import pallas as pl
from jax.experimental.pallas import tpu as pltpu
from jax.sharding import PartitionSpec as P


BLOCK_ROWS = 2
BLOCK_COLS = 128
STEP = 4

beta_one = 0.9
beta_two = 0.999
epsilon = 0.0001
root_half = 0.7978845608028654
cubic = 0.044715

F32 = jnp.float32
BF16 = jnp.bfloat16


def gelu_parts(value):
    square = value * value
    inner = root_half * (value + cubic * square * value)
    slope_inner = root_half * (1.0 + 3.0 * cubic * square)
    curve_inner = 6.0 * root_half * cubic * value
    tangent = jnp.tanh(inner)
    damping = 1.0 - tangent * tangent
    activated = 0.5 * value * (1.0 + tangent)
    slope = 0.5 * (1.0 + tangent) + 0.5 * value * damping * slope_inner
    bend = damping * slope_inner + 0.5 * value * damping * (
        curve_inner - 2.0 * tangent * slope_inner * slope_inner
    )
    return (activated, slope, bend)


def dot_nt(left, right):
    return lax.dot_general(left, right, (((1,), (1,)), ((), ())), preferred_element_type=F32)


def dot_tn(left, right):
    return lax.dot_general(left, right, (((0,), (0,)), ((), ())), preferred_element_type=F32)


def dot_nn(left, right):
    return jnp.dot(left, right, preferred_element_type=F32)


FORWARD_UNITS = 320
TILT_UNITS = 320
SPREAD_COLS = 512
BASE_UNITS = 160
TANGENT_UNITS = 320
UPDATE_UNITS = 320
FORWARD_LIMIT = 14
BASE_LIMIT = 25
TANGENT_LIMIT = 27
UPDATE_LIMIT = 9


def unit_block(units, wanted):
    return wanted if units % wanted == 0 else units


def whole(shape):
    zeros = (0,) * len(shape)
    return pl.BlockSpec(shape, lambda *_: zeros, pipeline_mode=pl.Buffered(1))


def in_vmem(array):
    return pltpu.with_memory_space_constraint(array, pltpu.VMEM)


def in_hbm(array):
    return pltpu.with_memory_space_constraint(array, pltpu.HBM)


HELD = pl.BlockSpec(memory_space=pltpu.VMEM)


def call(body, grid, in_specs, out_specs, out_shape, scratch, flops, traffic, limit, args, aliases={}):
    return pl.pallas_call(
        body,
        grid=grid,
        in_specs=in_specs,
        out_specs=out_specs,
        out_shape=out_shape,
        scratch_shapes=scratch,
        input_output_aliases=aliases,
        compiler_params=pltpu.CompilerParams(
            dimension_semantics=("arbitrary",) * len(grid), vmem_limit_bytes=limit * 1024 * 1024
        ),
        cost_estimate=pl.CostEstimate(flops=flops, bytes_accessed=traffic, transcendentals=0),
    )(*args)


def column_sums(values, kind, out):
    rows, width = values.shape
    lanes = lax.broadcasted_iota(jnp.int32, (rows, 128), 1)
    cols = width // BLOCK_COLS
    for at in range(cols):
        part = values[:, at * BLOCK_COLS : (at + 1) * BLOCK_COLS]
        out = jnp.where(lanes == kind * cols + at, jnp.sum(part, axis=1, keepdims=True), out)
    return out


def norm_kernel(tokens, gain, out):
    x = tokens[...].astype(F32)
    factor = lax.rsqrt(jnp.mean(x * x, axis=-1, keepdims=True) + 1e-06)
    out[...] = (x * factor * gain[...]).astype(BF16)


def norm(tokens, gain):
    rows, width = tokens.shape
    return call(
        norm_kernel,
        (1,),
        [whole((rows, width)), whole((1, width))],
        whole((rows, width)),
        jax.ShapeDtypeStruct((rows, width), BF16),
        [],
        rows * width * 4,
        rows * width * 4,
        8,
        (in_hbm(tokens), in_hbm(gain.reshape(1, width))),
    )


def joined(refs):
    return jnp.concatenate([ref[...] for ref in refs], axis=1)


def forward_kernel(pieces, chunk, refs):
    blocks = refs[:pieces]
    w = refs[pieces]
    (x, p_out, g_out, s_out, b_out, hid_out, own_q, sib_q, acc_q) = refs[-9:]
    step = pl.program_id(0)
    rows = blocks[0].shape[0]
    count = rows * pieces
    first_row = chunk * count

    @pl.when(step == 0)
    def _():
        for at in range(pieces):
            x[first_row + at * rows : first_row + (at + 1) * rows] = blocks[at][...]

    total, width = w.shape[1:]
    units = unit_block(total, FORWARD_UNITS)
    span = pl.ds(pl.multiple_of(step * units, 16), units)
    pre = dot_nt(w[0:2, span].reshape(2 * units, width), x[first_row : first_row + count])
    pre_gate, pre_up = (pre[:units], pre[units:])
    activated, slope, bend = gelu_parts(pre_gate)
    p_out[span] = pre_up * slope
    g_out[span] = activated
    s_out[span] = slope
    b_out[span] = pre_up * bend
    hidden = (activated * pre_up).astype(BF16)
    hid_out[span] = hidden
    quarter = acc_q.shape[1]
    first = pl.multiple_of(lax.axis_index("probe") * quarter, quarter)
    add_q = dot_tn(hidden, w[2, span, pl.ds(first, quarter)])

    @pl.when(step == 0)
    def _():
        acc_q[...] = add_q

    @pl.when(step > 0)
    def _():
        acc_q[...] += add_q

    @pl.when(step == pl.num_programs(0) - 1)
    def _():
        half = own_q.shape[0]
        own_q[...] = acc_q[:half]
        sib_q[...] = acc_q[half:].astype(sib_q.dtype)


def forward(blocks, weights, chunk, chunks, x, quarter, sib_type):
    rows, width = blocks[0].shape
    count = rows * len(blocks)
    units = weights.shape[1]
    ub = unit_block(units, FORWARD_UNITS)
    half = count // 2
    held = [] if x is None else [x]
    return call(
        lambda *refs: forward_kernel(len(blocks), chunk, refs),
        (units // ub,),
        [whole((rows, width))] * len(blocks) + [HELD] * (1 + len(held)),
        [HELD] * 8,
        [pltpu.VMEM((count * chunks, width), BF16)]
        + [pltpu.VMEM((units, count), F32)] * 4
        + [
            pltpu.VMEM((units, count), BF16),
            pltpu.VMEM((half, quarter), F32),
            pltpu.VMEM((half, quarter), sib_type),
        ],
        [pltpu.VMEM((count, quarter), F32)],
        2 * count * units * width * 2,
        units * width * 6 + units * count * 18 + count * width * 4,
        FORWARD_LIMIT,
        (*blocks, in_vmem(weights), *map(in_vmem, held)),
        {len(blocks) + 1: 0} if held else {},
    )


def tilt_kernel(chunk, z, x, p, g, s, b, q_out, s_out, tan_out):
    total, width = z.shape[1:]
    units = unit_block(total, TILT_UNITS)
    count = p.shape[1]
    span = pl.ds(pl.multiple_of(pl.program_id(0) * units, 16), units)
    rows = slice(chunk * count, (chunk + 1) * count)
    tan = dot_nt(z[0:2, span].reshape(2 * units, width), x[rows])
    tan_gate, tan_up = (tan[:units], tan[units:])
    slope = s[span]
    q_out[span] = tan_up * slope + b[span] * tan_gate
    s_out[span] = slope * tan_gate
    tan_out[span] = (p[span] * tan_gate + g[span] * tan_up).astype(BF16)


def tilt(signs, chunk, x, p, g, s, b):
    units, count = p.shape
    width = x.shape[1]
    ub = unit_block(units, TILT_UNITS)
    return call(
        functools.partial(tilt_kernel, chunk),
        (units // ub,),
        [HELD] * 6,
        [HELD] * 3,
        [pltpu.VMEM((units, count), F32)] * 2 + [pltpu.VMEM((units, count), BF16)],
        [],
        2 * count * units * width * 2,
        units * width * 4 + units * count * 26 + count * width * 2,
        FORWARD_LIMIT,
        tuple(map(in_vmem, (signs, x, p, g, s, b))),
    )


def spread_kernel(parts, refs):
    (w, z) = refs[:2]
    tans = refs[2 : 2 + parts]
    hids = refs[2 + parts : 2 + 2 * parts]
    (own, sib, left) = refs[2 + 2 * parts :]
    units, count = hids[0].shape
    step = pl.program_id(0)

    @pl.when(step == 0)
    def _():
        for at in range(parts):
            span = slice(at * count, (at + 1) * count)
            left[span, :units] = tans[at][...].T
            left[span, units:] = hids[at][...].T

    cols = min(SPREAD_COLS, own.shape[1])
    span = pl.ds(pl.multiple_of(step * cols, cols), cols)
    total = dot_nn(left[...], jnp.concatenate([w[2, :, span], z[2, :, span]], axis=0))
    half = count // 2
    for at in range(parts):
        top = at * count
        rows = slice(at * half, (at + 1) * half)
        own[rows, span] = total[top : top + half]
        sib[rows, span] = total[top + half : top + count].astype(sib.dtype)


def spread(weights, signs, tans, hids, sib_type):
    units, count = hids[0].shape
    parts = len(hids)
    width = weights.shape[2]
    half = parts * count // 2
    cols = SPREAD_COLS
    return call(
        lambda *refs: spread_kernel(parts, refs),
        (width // cols,),
        [HELD] * (2 + 2 * parts),
        [HELD, HELD],
        [pltpu.VMEM((half, width), F32), pltpu.VMEM((half, width), sib_type)],
        [pltpu.VMEM((parts * count, 2 * units), BF16)],
        4 * parts * count * units * width,
        units * width * 4 + half * width * 6,
        FORWARD_LIMIT,
        tuple(map(in_vmem, (weights, signs, *tans, *hids))),
    )


def fold_kernel(parts, rows, refs):
    owns = refs[:parts]
    gots = refs[parts : 2 * parts]
    outs = refs[2 * parts :]
    at = 0
    for own, got in zip(owns, gots):
        for first in range(0, own.shape[0], rows):
            span = slice(first, first + rows)
            outs[at][...] = (own[span] + got[span].astype(F32)).astype(outs[at].dtype)
            at += 1


def fold(owns, gots, rows, keep):
    parts = len(owns)
    blocks = sum(own.shape[0] for own in owns) // rows
    width = owns[0].shape[1]
    return call(
        lambda *refs: fold_kernel(parts, rows, refs),
        (1,),
        [HELD] * (2 * parts),
        [HELD] * blocks,
        [pltpu.VMEM((rows, width), F32 if keep and at == 0 else BF16) for at in range(blocks)],
        [],
        rows * blocks * width * 64,
        rows * blocks * width * 8,
        8,
        tuple(map(in_vmem, (*owns, *gots))),
    )


def load_kernel(plan, refs):
    count = len(plan)
    (sources, targets, sems) = (refs[:count], refs[count : 2 * count], refs[2 * count])
    copies = []
    for source, target, picks in zip(sources, targets, plan):
        for place, pick in enumerate(picks):
            copies.append(
                pltpu.make_async_copy(source.at[pick], target.at[place], sems.at[len(copies)])
            )
    for copy in copies:
        copy.start()
    for copy in copies:
        copy.wait()


def load(arrays, plan):
    shapes = [(len(picks), *array.shape[1:]) for array, picks in zip(arrays, plan)]
    size = sum(math.prod(dims) for dims in shapes)
    return pl.pallas_call(
        lambda *refs: load_kernel(plan, refs),
        name="load",
        in_specs=[pl.BlockSpec(memory_space=pltpu.HBM)] * len(arrays),
        out_specs=[HELD] * len(arrays),
        out_shape=[pltpu.VMEM(dims, array.dtype) for dims, array in zip(shapes, arrays)],
        scratch_shapes=[pltpu.SemaphoreType.DMA((sum(map(len, plan)),))],
        compiler_params=pltpu.CompilerParams(vmem_limit_bytes=8 * 1024 * 1024),
        cost_estimate=pl.CostEstimate(
            flops=size * 64, bytes_accessed=size * 8, transcendentals=0
        ),
    )(*map(in_hbm, arrays))


def load_moment(array):
    kinds, units, width = array.shape
    ub = unit_block(units, BASE_UNITS)
    split = array.reshape(kinds * units // ub, ub, width)
    return load([split], [tuple(range(split.shape[0]))])[0]


def load_weights(weights, signs):
    kinds, units, width = weights.shape
    halves = 2 if units % 32 == 0 else 1
    dims = (kinds * halves, units // halves, width)
    picks = tuple(range(kinds * halves))
    loaded = load([weights.reshape(dims), signs.reshape(dims)], [picks, picks])
    return [array.reshape(kinds, units, width) for array in loaded]


def joined(refs, span):
    return jnp.concatenate([ref[span] for ref in refs], axis=1)


def base_kernel(pieces, parts, refs):
    blocks = refs[: 2 * pieces]
    refs = refs[2 * pieces :]
    (w, z, m, normed) = refs[:4]
    groups = [refs[4 + at * parts : 4 + (at + 1) * parts] for at in range(6)]
    (ps, gs, qs, ss, hids, tans) = groups
    (new_m, held, e_gate, e_up, sums, dout) = refs[4 + 6 * parts :]
    step = pl.program_id(0)
    half, quarter = blocks[0].shape
    chunk = 2 * half // parts

    @pl.when(step == 0)
    def _():
        me = lax.axis_index("probe")
        for at in range(pieces):
            first = pl.multiple_of((me ^ at) * quarter, quarter)
            for side in range(2):
                source = blocks[side * pieces + at]
                for part in range(parts):
                    start = part * chunk + side * (chunk // 2)
                    dout[start : start + chunk // 2, pl.ds(first, quarter)] = source[
                        part * (chunk // 2) : (part + 1) * (chunk // 2)
                    ]

    units = w.shape[1]
    kinds = new_m.shape[0]
    blocks_of = m.shape[0] // kinds
    span = pl.ds(pl.multiple_of(step * units, 16), units)
    d = dout[...]
    both = dot_nt(jnp.concatenate([w[0], z[0, 0]], axis=0), d)
    dhid, sdhid = (both[:units], both[units:])
    pv, gv = (joined(ps, span), joined(gs, span))
    e_gate[span] = sdhid * pv + dhid * joined(qs, span)
    e_up[span] = sdhid * gv + dhid * joined(ss, span)
    inner = jnp.concatenate([(dhid * pv).astype(BF16), (dhid * gv).astype(BF16)], axis=0)
    grads = dot_nn(inner, normed[...])

    def moment(kind, grad):
        at = kind * blocks_of + step
        value = beta_one * m[at] + (1.0 - beta_one) * grad
        new_m[kind] = value
        held[at] = value

    moment(0, grads[:units])
    moment(1, grads[units:])
    outer = dot_nn(jnp.concatenate([joined(hids, span), joined(tans, span)], axis=0), d)
    moment(2, outer[:units])
    sums[span] = column_sums(z[0, 0].astype(F32) * outer[units:], 2, jnp.zeros((units, 128), F32))


def base(pieces, weights, signs, m, x, ps, gs, qs, ss, hids, tans):
    half, quarter = pieces[0].shape
    kinds, units, width = weights.shape
    count = 2 * half
    parts = len(ps)
    ub = unit_block(units, BASE_UNITS)
    return call(
        lambda *refs: base_kernel(len(pieces) // 2, parts, refs),
        (units // ub,),
        [whole((half, quarter))] * len(pieces)
        + [
            pl.BlockSpec((1, ub, width), lambda i: (2, i, 0)),
            pl.BlockSpec((1, 1, ub, width), lambda i: (0, 2, i, 0)),
        ]
        + [HELD] * (2 + 6 * parts),
        [pl.BlockSpec((kinds, ub, width), lambda i: (0, i, 0))] + [HELD] * 4,
        [
            jax.ShapeDtypeStruct((kinds, units, width), F32),
            pltpu.VMEM(m.shape, F32),
            pltpu.VMEM((units, count), F32),
            pltpu.VMEM((units, count), F32),
            pltpu.VMEM((units, 128), F32),
        ],
        [pltpu.VMEM((count, width), BF16)],
        2 * count * units * width * 6,
        units * width * 28 + units * count * 28,
        BASE_LIMIT,
        (
            *pieces,
            in_hbm(weights),
            in_hbm(signs),
            *map(in_vmem, (m, x, *ps, *gs, *qs, *ss, *hids, *tans)),
        ),
        {len(pieces) + 2: 1},
    )


def tangent_kernel(pieces, parts, refs):
    blocks = refs[:pieces]
    (w, z, normed, e_gate, e_up, sums_in) = refs[pieces : pieces + 6]
    refs = refs[pieces + 6 :]
    (ps, gs, hids) = [refs[at * parts : (at + 1) * parts] for at in range(3)]
    (sums, tdout, rows_sum, pairs) = refs[3 * parts :]
    step = pl.program_id(0)
    rows = blocks[0].shape[0]

    @pl.when(step == 0)
    def _():
        for at in range(pieces):
            tdout[at * rows : (at + 1) * rows] = blocks[at][...]

    units = w.shape[1]
    span = pl.ds(pl.multiple_of(step * units, 16), units)
    t = tdout[...]
    tdh = dot_nt(w[0], t)
    inner = jnp.concatenate(
        [
            (tdh * joined(ps, span) + e_gate[span]).astype(BF16),
            (tdh * joined(gs, span) + e_up[span]).astype(BF16),
        ],
        axis=0,
    )
    hv = dot_nn(inner, normed[...])
    hv_out = dot_nn(joined(hids, span), t)
    made = jnp.zeros((units, 128), F32)
    made = column_sums(z[0, 0].astype(F32) * hv[:units], 0, made)
    made = column_sums(z[0, 1].astype(F32) * hv[units:], 1, made)
    made = column_sums(z[0, 2].astype(F32) * hv_out, 2, made)
    rows_sum[...] = made + sums_in[span]
    half = units // BLOCK_ROWS
    pairs[pl.ds(pl.multiple_of(step * half, 8), half), :] = (
        rows_sum[pl.ds(0, half, stride=2), :] + rows_sum[pl.ds(1, half, stride=2), :]
    )

    @pl.when(step == pl.num_programs(0) - 1)
    def _():
        sums[...] = pairs[...].T[: sums.shape[0]]


def tangent(blocks, weights, signs, normed, e_gate, e_up, sums, ps, gs, hids):
    rows, width = blocks[0].shape
    count = normed.shape[0]
    kinds, units, _ = weights.shape
    parts = len(ps)
    ub = unit_block(units, TANGENT_UNITS)
    cols = width // BLOCK_COLS
    return call(
        lambda *refs: tangent_kernel(len(blocks), parts, refs),
        (units // ub,),
        [whole((rows, width))] * len(blocks)
        + [
            pl.BlockSpec((1, ub, width), lambda i: (2, i, 0)),
            pl.BlockSpec((1, kinds, ub, width), lambda i: (0, 0, i, 0)),
        ]
        + [HELD] * (4 + 3 * parts),
        whole((kinds * cols, units // BLOCK_ROWS)),
        jax.ShapeDtypeStruct((kinds * cols, units // BLOCK_ROWS), F32),
        [
            pltpu.VMEM((count, width), BF16),
            pltpu.VMEM((ub, 128), F32),
            pltpu.VMEM((units // BLOCK_ROWS, 128), F32),
        ],
        2 * count * units * width * 4,
        units * width * 8 + units * count * 18,
        TANGENT_LIMIT,
        (
            *blocks,
            in_hbm(weights),
            in_hbm(signs),
            *map(in_vmem, (normed, e_gate, e_up, sums, *ps, *gs, *hids)),
        ),
    )


def update_kernel(probes, a, b, c, d, v, m, hess, new_v, update, scales):
    kinds, cols, half = v.shape
    kind, step = (pl.program_id(0), pl.program_id(1))

    @pl.when((kind == 0) & (step == 0))
    def _():
        total = (a[...] + b[...]) + (c[...] + d[...])
        for at in range(kinds):
            h = total[at * cols : (at + 1) * cols] * (1.0 / (BLOCK_ROWS * BLOCK_COLS * probes))
            hess[at] = h
            nv = beta_two * v[at] + (1.0 - beta_two) * h * h
            new_v[at] = nv
            denom = jnp.sqrt(nv / (1.0 - beta_two**STEP)) + epsilon
            scale = 1.0 / (denom * (1.0 - beta_one**STEP))
            wide = jnp.concatenate([scale, jnp.zeros((128 - cols, half), F32)], axis=0).T
            scales[at, pl.ds(0, half, stride=2), :] = wide
            scales[at, pl.ds(1, half, stride=2), :] = wide

    tall = update.shape[1]
    full = scales[kind, pl.ds(pl.multiple_of(step * tall, tall), tall), :]
    pieces = tall // m.shape[1]
    first = (kind * pl.num_programs(1) + step) * pieces
    for piece in range(pieces):
        rows = slice(piece * m.shape[1], (piece + 1) * m.shape[1])
        for at in range(cols):
            span = slice(at * BLOCK_COLS, (at + 1) * BLOCK_COLS)
            update[0, rows, span] = m[first + piece, :, span] * full[rows, at : at + 1]


def update_step(sums, v, m):
    kinds, _, half = v.shape
    units, width = (half * BLOCK_ROWS, m.shape[2])
    ub = unit_block(units, UPDATE_UNITS)
    m_spec = pl.BlockSpec((1, ub, width), lambda k, i: (k, i, 0))
    shape = jax.ShapeDtypeStruct
    return call(
        functools.partial(update_kernel, len(sums)),
        (kinds, units // ub),
        [whole(sums[0].shape)] * 4 + [whole(v.shape), pl.BlockSpec(memory_space=pltpu.VMEM)],
        [whole(v.shape), whole(v.shape), m_spec],
        [shape(v.shape, F32), shape(v.shape, F32), shape((kinds, units, width), F32)],
        [pltpu.VMEM((kinds, units, 128), F32)],
        units * width * 6,
        units * width * 24,
        UPDATE_LIMIT,
        (*sums, v, in_vmem(m)),
    )


def to_sibling(x, chips):
    return lax.ppermute(x, "mp", [(i, i ^ 1) for i in range(2 * chips)])


def to_chip(x, chips, flip):
    pairs = [(2 * z + c, 2 * (z ^ flip) + c) for z in range(chips) for c in range(2)]
    return lax.ppermute(x, "mp", pairs)


def to_probe(x, probes, flip):
    return lax.ppermute(x, "probe", [(i, i ^ flip) for i in range(probes)])


def gather_rows(x, chips):
    own = [x]
    for flip in range(1, chips):
        own.append(to_chip(x, chips, flip))
    sib = []
    for flip in range(chips):
        sib.append(to_sibling(own[flip], chips))
    half = chips // 2
    return [own[:half] + sib[:half], own[half:] + sib[half:]]


def near_path(normed, offset, weights, probe_signs, m_state, chips, probes):
    rows, width = normed.shape
    count = 2 * chips * rows
    quarter = width // probes
    chunks = gather_rows(normed, chips)
    w, z = load_weights(weights, probe_signs)
    x = None
    ps, gs, qs, ss, hids, tans, folded = ([], [], [], [], [], [], [])
    for at, blocks in enumerate(chunks):
        x, p, g, s, b, hid, own_q, sib_q = forward(
            blocks, w, at, len(chunks), x, quarter, BF16
        )
        got = to_sibling(sib_q, chips)
        folded += fold([own_q], [got], rows, at == 0)
        q, s, tan = tilt(z, at, x, p, g, s, b)
        for held, value in zip((ps, gs, qs, ss, hids, tans), (p, g, q, s, hid, tan)):
            held.append(value)
    own_t, sib_t = spread(w, z, tans, hids, BF16)
    kept, *sent = folded
    kept = kept + offset
    for flip in range(1, chips):
        kept = kept + to_chip(sent[flip - 1], chips, flip).astype(F32)
    part = (kept / count).astype(BF16)
    mine = [part]
    for flip in range(1, chips):
        mine.append(to_chip(part, chips, flip))
    mine = jnp.concatenate(mine, axis=0)
    pieces = [mine]
    for flip in range(1, probes):
        pieces.append(to_probe(mine, probes, flip))
    for at in range(probes):
        pieces.append(to_sibling(pieces[at], chips))
    got = to_sibling(sib_t, chips)
    kept, *sent = fold([own_t], [got], rows, True)
    for flip in range(1, chips):
        kept = kept + to_chip(sent[flip - 1], chips, flip).astype(F32)
    tan_dout = (kept / count).astype(BF16)
    tan_blocks = gather_rows(tan_dout, chips)
    held = load_moment(m_state)
    new_m, held, e_gate, e_up, sums = base(
        pieces, weights, probe_signs, held, x, ps, gs, qs, ss, hids, tans
    )
    sums = tangent(
        tan_blocks[0] + tan_blocks[1],
        weights,
        probe_signs,
        x,
        e_gate,
        e_up,
        sums,
        ps,
        gs,
        hids,
    )
    return new_m, held, sums


def far_path(normed, offset, weights, probe_signs, m_state, chips, probes):
    rows, width = normed.shape
    count = 2 * chips * rows
    quarter = width // probes
    blocks = [lax.all_gather(normed, "mp", axis=0, tiled=True)]
    w, z = load_weights(weights, probe_signs)
    x, p, g, s, b, hid, own_q, sib_q = forward(blocks, w, 0, 1, None, quarter, F32)
    q, s, tan = tilt(z, 0, x, p, g, s, b)
    own_t, sib_t = spread(w, z, [tan], [hid], F32)
    part = lax.psum_scatter(
        jnp.concatenate([own_q, sib_q], axis=0), "mp", scatter_dimension=0, tiled=True
    )
    mine = lax.all_gather(
        ((part + offset) / count).astype(BF16), "mp", axis=0, tiled=True
    )
    pieces = [mine] + [to_probe(mine, probes, flip) for flip in range(1, probes)]
    half = count // 2
    pieces = [piece[:half] for piece in pieces] + [piece[half:] for piece in pieces]
    kept = lax.psum_scatter(
        jnp.concatenate([own_t, sib_t], axis=0), "mp", scatter_dimension=0, tiled=True
    )
    tan_blocks = [lax.all_gather((kept / count).astype(BF16), "mp", axis=0, tiled=True)]
    held = load_moment(m_state)
    new_m, held, e_gate, e_up, sums = base(
        pieces, weights, probe_signs, held, x, [p], [g], [q], [s], [hid], [tan]
    )
    sums = tangent(
        tan_blocks, weights, probe_signs, x, e_gate, e_up, sums, [p], [g], [hid]
    )
    return new_m, held, sums


def shards(tokens, targets, norm_gain, weights, probe_signs, m_state, v_state):
    probes = lax.axis_size("probe")
    chips = lax.axis_size("mp") // 2
    quarter = tokens.shape[1] // probes
    first = lax.axis_index("probe") * quarter
    normed = norm(tokens, norm_gain)
    offset = lax.dynamic_slice_in_dim(tokens, first, quarter, 1).astype(
        F32
    ) - lax.dynamic_slice_in_dim(targets, first, quarter, 1).astype(F32)
    path = near_path if chips == 4 else far_path
    new_m, held, sums = path(normed, offset, weights, probe_signs, m_state, chips, probes)
    sums = [sums] + [to_probe(sums, probes, flip) for flip in range(1, probes)]
    hess, new_v, update = update_step(sums, v_state.transpose(0, 2, 1), held)
    return (hess.transpose(0, 2, 1), new_m, new_v.transpose(0, 2, 1), update)


def solution(mesh):
    return jax.shard_map(
        shards,
        mesh=mesh,
        in_specs=(
            P("mp", None),
            P("mp", None),
            P(),
            P(None, "mp", None),
            P("probe", None, "mp", None),
            P(None, "mp", None),
            P(None, "mp", None),
        ),
        out_specs=(
            P(None, "mp", None),
            P(None, "mp", None),
            P(None, "mp", None),
            P(None, "mp", None),
        ),
        check_vma=False,
    )
```
